32 devices in a mesh: ta: 2 (over x), gz: 4 (over y, core), gy: 4 (over z).
Axes of the slice: x: 2, y: 2, z: 4, core: 2. Of those that a mesh axis runs over, the one named last changes fastest.
Arguments:
- propagator: bfloat16 [2, 4, 3, 12, 2, 4, 512], P(None, None, None, None, 'ta', 'gz', 'gy'), may hold values from -6 to 6
- links: bfloat16 [2, 3, 3, 2, 4, 512], P(None, None, None, 'ta', 'gz', 'gy'), may hold values from -2.5 to 2.5
- source_z: int32 [2, 4], replicated, may hold values from 0 to 3
- displacements: int32 [3], replicated, may hold values from 0 to 2, each once
- momenta: int32 [4], replicated, may hold values from 1 to 3
- gamma_perm: int32 [4, 4], replicated, may hold values from 0 to 3, each once within a row
- gamma_phase: int32 [4, 4], replicated, may hold values from 0 to 3
Outputs:
- correlator: float32 [2, 3, 4, 4, 2], replicated
The draws below stay inside these ranges and needn't reach their ends.
Inputs may be any that keep to these rules, and one draw needn't show every extreme that they name: `displacements`: every displacement from -1 to 1 appears exactly once. `gamma_perm`: each row is a permutation of the four spin indices.
All inputs are finite; a program needn't handle non-finite values.
Results may differ from the reference program's by a relative error of at most 0.0003.
Values may be sent and summed in bfloat16 or wider, within the bound.
A program may use at most 64 MiB of HBM per device.

```python
import math
import jax
import jax.numpy as jnp
from jax import lax

NX = 64
NG = 4
NP = 4
NSTEP = 1
NDISP = 3
NT = 2
NZ = 4
NY = 8
NYX = 512


def with_ends(array, rng, least, largest):
    longest = array.shape.index(max(array.shape))
    spots = []
    for shift in (0, 1):
        where = [jax.random.randint(jax.random.fold_in(rng, axis), (), 0, length) for axis, length in enumerate(array.shape)]
        where[longest] = (where[longest] + shift) % array.shape[longest]
        spots.append(tuple(where))
    return array.at[spots[0]].set(least).at[spots[1]].set(largest)


def block_levels(rng, dims, shards, least, high):
    level, own = 1.0, jax.random.fold_in(rng, 6)
    for axis_at, blocks in shards:
        steps = jnp.exp(jax.random.uniform(jax.random.fold_in(own, axis_at), (blocks,), jnp.float32, least / len(shards), high / len(shards)))
        level = level * jnp.repeat(steps, dims[axis_at] // blocks).reshape([-1 if axis == axis_at else 1 for axis in range(len(dims))])
    return level


def centred(own_key, extent, width, most, split=(), held_as=jnp.bfloat16):
    gain = block_levels(own_key, extent, split, -0.22, 0.18) if split else 1.0
    array = jax.random.normal(own_key, extent, jnp.float32) * width * gain
    return jnp.minimum(jnp.maximum(array, -most), most).astype(held_as)


def setup_inputs(seed: int = 0) -> dict:
    key_of = jax.random.split(jax.random.key(seed), 8)
    return {
        "propagator": centred(key_of[0], (2, 4, 3, 12, NT, NZ, NYX), 1.0, 6.0, ((4, 2), (5, 4), (6, 4))),
        "links": centred(key_of[1], (2, 3, 3, NT, NZ, NYX), 6 ** -0.5, 2.5, ((3, 2), (4, 4), (5, 4))),
        "source_z": with_ends(jax.random.randint(key_of[2], (NT, NP), 0, NZ), jax.random.fold_in(key_of[2], 1), 0, NZ - 1).astype(jnp.int32),
        "displacements": jax.random.permutation(key_of[3], NDISP).astype(jnp.int32),
        "momenta": with_ends(jax.random.randint(key_of[4], (NP,), 1, 4), jax.random.fold_in(key_of[4], 1), 1, 3).astype(jnp.int32),
        "gamma_perm": jax.vmap(lambda own: jax.random.permutation(own, 4))(jax.random.split(key_of[5], NG)).reshape((NG, 4)).astype(jnp.int32),
        "gamma_phase": with_ends(jax.random.randint(key_of[6], (NG, 4), 0, 4), jax.random.fold_in(key_of[6], 1), 0, 3).astype(jnp.int32),
    }


highest = lax.Precision.HIGHEST

def colour_apply(wilson, field_now):
    form = 'ab...,sbc...->sac...'
    real_part = jnp.einsum(form, wilson[0], field_now[0], precision=highest) - jnp.einsum(form, wilson[1], field_now[1], precision=highest)
    imag_part = jnp.einsum(form, wilson[0], field_now[1], precision=highest) + jnp.einsum(form, wilson[1], field_now[0], precision=highest)
    return jnp.stack([real_part, imag_part])

def link_product(left_link, right_link):
    form = 'ab...,bc...->ac...'
    real_part = jnp.einsum(form, left_link[0], right_link[0], precision=highest) - jnp.einsum(form, left_link[1], right_link[1], precision=highest)
    imag_part = jnp.einsum(form, left_link[0], right_link[1], precision=highest) + jnp.einsum(form, left_link[1], right_link[0], precision=highest)
    return jnp.stack([real_part, imag_part])

def dagger(link_field):
    return jnp.stack([jnp.swapaxes(link_field[0], 0, 1), -jnp.swapaxes(link_field[1], 0, 1)])

def spin_pairs(source, field_now):
    form = 'sac...,uac...->su...'
    real_part = jnp.einsum(form, source[0], field_now[0], precision=highest) + jnp.einsum(form, source[1], field_now[1], precision=highest)
    imag_part = jnp.einsum(form, source[0], field_now[1], precision=highest) - jnp.einsum(form, source[1], field_now[0], precision=highest)
    return (real_part, imag_part)

def insert(gamma_real, gamma_imag, pairs):
    pair_real, pair_imag = pairs
    form = 'gsu,su...->g...'
    real_part = jnp.einsum(form, gamma_real, pair_real, precision=highest) - jnp.einsum(form, gamma_imag, pair_imag, precision=highest)
    imag_part = jnp.einsum(form, gamma_real, pair_imag, precision=highest) + jnp.einsum(form, gamma_imag, pair_real, precision=highest)
    return (real_part, imag_part)

def gamma_tables(gamma_perm, gamma_phase):
    columns = jnp.arange(4, dtype=jnp.int32)
    hits = (gamma_perm[:, :, None] == columns[None, None, :]).astype(jnp.float32)
    real_part = (gamma_phase == 0).astype(jnp.float32) - (gamma_phase == 2).astype(jnp.float32)
    imag_part = (gamma_phase == 1).astype(jnp.float32) - (gamma_phase == 3).astype(jnp.float32)
    return (hits * real_part[:, :, None], hits * imag_part[:, :, None])

def reference(propagator, links, source_z, displacements, momenta, gamma_perm, gamma_phase):
    gamma_real, gamma_imag = gamma_tables(gamma_perm, gamma_phase)
    depth_index = jnp.arange(NZ, dtype=jnp.int32)
    turn_count = momenta[None, :, None] * (depth_index[None, None, :] - source_z[:, :, None]) % NZ
    angles = turn_count.astype(jnp.float32) * (2.0 * math.pi / NZ)
    cosine_all = jnp.cos(angles)
    sine_all = jnp.sin(angles)
    scaling = 1.0 / (24.0 * math.sqrt(NX * NY * NZ))
    unit = jnp.broadcast_to(jnp.eye(3, dtype=jnp.float32)[:, :, None, None], (3, 3, NZ, NYX))
    identity = jnp.stack([unit, jnp.zeros_like(unit)])

    def one_slice(slice_pack):
        source = slice_pack[0].astype(jnp.float32)
        link_field = slice_pack[1].astype(jnp.float32)
        cosine = slice_pack[2]
        sine_table = slice_pack[3]

        def project(field_now):
            trace_real, trace_imag = insert(gamma_real, gamma_imag, spin_pairs(source, field_now))
            line_real = lax.optimization_barrier(jnp.sum(trace_real, axis=-1))
            line_imag = lax.optimization_barrier(jnp.sum(trace_imag, axis=-1))
            real_part = jnp.dot(line_real, cosine.T, precision=highest) + jnp.dot(line_imag, sine_table.T, precision=highest)
            imag_part = jnp.dot(line_imag, cosine.T, precision=highest) - jnp.dot(line_real, sine_table.T, precision=highest)
            return jnp.stack([real_part, imag_part], axis=-1) * scaling
        results = {0: project(source)}
        wilson = identity
        for reach in range(1, NSTEP + 1):
            wilson = link_product(wilson, jnp.roll(link_field, -(reach - 1), axis=3))
            results[reach] = project(colour_apply(wilson, jnp.roll(source, -reach, axis=4)))
        wilson = identity
        for reach in range(1, NSTEP + 1):
            wilson = link_product(wilson, dagger(jnp.roll(link_field, reach, axis=3)))
            results[-reach] = project(colour_apply(wilson, jnp.roll(source, reach, axis=4)))
        return jnp.stack([results[offset] for offset in range(-NSTEP, NSTEP + 1)])
    slices = lax.map(one_slice, (jnp.moveaxis(propagator, 4, 0), jnp.moveaxis(links, 3, 0), cosine_all, sine_all))
    return jnp.take(slices, displacements.astype(jnp.int32), axis=1)
```

```python
import functools
import math

import jax
import jax.numpy as jnp
from jax import lax
from jax.experimental import pallas as pl
from jax.experimental.pallas import tpu as pltpu
from jax.sharding import PartitionSpec as P

MESH = pl.DeviceIdType.MESH
LANES = 128


def weights(lane_row, sizes, smem, place, scaling):
    ndisp, ng, np_, nz = sizes
    src, disp, mom, perm, phase = smem
    slice_at, depth_at = place
    nsteps = (ndisp - 1) // 2
    shape = (32, LANES)
    lane = lax.broadcasted_iota(jnp.int32, shape, 1) + lane_row * LANES
    row = lax.broadcasted_iota(jnp.int32, shape, 0)
    momentum = lane & (np_ - 1)
    out_part = (lane // np_) & 1
    gamma = (lane // (2 * np_)) & (ng - 1)
    entry = lane // (2 * np_ * ng)
    in_part = row // 16
    first = (row // 4) & 3
    second = row & 3
    reach = jnp.full(shape, 2 * nsteps + 1, jnp.int32)
    for j in range(ndisp):
        reach = jnp.where(entry == j, disp[j] - nsteps, reach)
    backward = reach < 0
    momenta = jnp.zeros(shape, jnp.int32)
    source = jnp.zeros(shape, jnp.int32)
    for p in range(np_):
        momenta = jnp.where(momentum == p, mom[p], momenta)
        source = jnp.where(momentum == p, src[slice_at, p], source)
    depth = depth_at - jnp.where(backward, reach, 0)
    turns = (momenta * (depth - source)).astype(jnp.float32) * (1.0 / nz)
    angle = (turns - jnp.floor(turns)) * (2.0 * math.pi)
    cosine = jnp.cos(angle)
    sine = jnp.sin(angle)
    sink = jnp.where(backward, second, first)
    other = jnp.where(backward, first, second)
    column = jnp.zeros(shape, jnp.int32)
    power = jnp.zeros(shape, jnp.int32)
    for g in range(ng):
        for s in range(4):
            here = (gamma == g) & (sink == s)
            column = jnp.where(here, perm[g, s], column)
            power = jnp.where(here, phase[g, s], power)
    quarter = power - out_part + jnp.where(backward, -in_part, in_part)
    quarter = quarter & 3
    value = jnp.where((quarter & 1) == 0, cosine, sine)
    value = jnp.where(quarter >= 2, -value, value)
    value = jnp.where((column == other) & (entry < ndisp), value * scaling, 0.0)
    return value, jnp.abs(reach)


def add_pairs(sums, left, turned, right, start, size):
    def rows(ref, s):
        return ref[pl.ds(start + s, size // 4, stride=4), :].reshape(-1, 8, LANES)

    rights = [rows(right, u) for u in range(4)]
    out = []
    for side in (left, turned):
        for s in range(4):
            own = rows(side, s)
            out += [jnp.sum(own * other, axis=0) for other in rights]
    return out if sums is None else [x + y for x, y in zip(sums, out)]


def site_sums(sums):
    stacked = jnp.concatenate([jnp.sum(x, axis=0, keepdims=True) for x in sums], axis=0)
    return jnp.sum(stacked, axis=1, keepdims=True)


def keep(left, turned, at, size, real, imag):
    real, imag = real.reshape(-1, LANES), imag.reshape(-1, LANES)
    left[pl.ds(at, size), :] = real
    left[pl.ds(at + size, size), :] = imag
    if turned is not None:
        turned[pl.ds(at, size), :] = -imag
        turned[pl.ds(at + size, size), :] = real


def kernel(
    sizes, scaling, ranks,
    prop, links, src_h, disp_h, mom_h, perm_h, phase_h,
    out,
    near, near_links, far, far_links, left, turned, right,
    src, disp, mom, perm, phase,
    gathered,
    local_sem, s_send, s_recv, a_send, a_recv, low_sem, line_sem, plane_sem, *link_sems,
):
    ndisp, ng, np_, nz = sizes
    nta, ngz, ngy = ranks
    nsteps = (ndisp - 1) // 2
    size = near.shape[2]
    lane_rows = gathered.shape[1]
    ta, gz, gy = lax.axis_index("ta"), lax.axis_index("gz"), lax.axis_index("gy")
    place = (ta * ngz + gz) * ngy + gy

    loads = [
        pltpu.make_async_copy(a, b, local_sem.at[i])
        for i, (a, b) in enumerate(
            [(prop, near), (links, near_links), (src_h, src), (disp_h, disp),
             (mom_h, mom), (perm_h, perm), (phase_h, phase)]
        )
    ]
    for load in loads:
        load.start()

    lines = [
        (gz, ngz, lambda i: (ta, i, gy)),
        (gy, ngy, lambda i: (ta, gz, i)),
        (ta, nta, lambda i: (i, gz, gy)),
    ]

    def greet(semaphore, at):
        pl.semaphore_signal(semaphore, inc=1, device_id=at, device_id_type=MESH)

    def greet_span(semaphore, line, low, high):
        lax.fori_loop(low, high, lambda i, carry: (greet(semaphore, line[2](i)), carry)[1], 0)

    def greet_line(semaphore, line):
        greet_span(semaphore, line, 0, line[0])
        greet_span(semaphore, line, line[0] + 1, line[1])

    count = nta * ngz * ngy
    barrier = pltpu.get_barrier_semaphore()
    for k in range(1, nsteps + 1):
        @pl.when(gz + k >= ngz)
        def _():
            greet(barrier, (ta, gz + k - ngz, gy))
    for line in lines:
        greet_span(barrier, line, line[0] + 1, line[1])
    nroots = min(2, ngz)
    is_root = (ta + gy == 0) & (gz < nroots)

    @pl.when(is_root)
    def _():
        def one(step, carry):
            at = (step // (ngz * ngy), step // ngy % ngz, step % ngy)

            @pl.when(step != place)
            def _():
                greet(barrier, at)

            return carry

        lax.fori_loop(0, count, one, 0)

    pl.semaphore_wait(
        barrier,
        jnp.maximum(gz, nsteps) + gy + ta + nroots - jnp.where(is_root, 1, 0),
    )
    for line in lines:
        greet_span(low_sem.at[0], line, 0, line[0])

    def target(k):
        return (ta, lax.rem(gz + ngz - k, ngz), gy)

    sends = [
        [
            pltpu.make_async_remote_copy(
                src_ref=near.at[:, c], dst_ref=far.at[k - 1, :, c], send_sem=s_send.at[0],
                recv_sem=s_recv.at[k - 1, c], device_id=target(k), device_id_type=MESH)
            for c in range(3)
        ]
        for k in range(1, nsteps + 1)
    ]
    u_send, u_recv = link_sems if link_sems else (None, None)
    link_sends = [
        pltpu.make_async_remote_copy(
            src_ref=near_links, dst_ref=far_links.at[k - 1], send_sem=u_send.at[k - 1],
            recv_sem=u_recv.at[k - 1], device_id=target(k), device_id_type=MESH)
        for k in range(1, nsteps)
    ]
    loads[0].wait()
    for c in range(3):
        for copies in sends:
            copies[c].start()
    loads[1].wait()
    for copy in link_sends:
        copy.start()
    for load in loads[2:]:
        load.wait()

    sums = None
    for c in range(3):
        keep(left, turned, 2 * size * c, size, near[0, c].astype(jnp.float32), near[1, c].astype(jnp.float32))
        sums = add_pairs(sums, left, turned, left, 2 * size * c, 2 * size)
    totals = [site_sums(sums)]
    later = (ngz - 1 - gz) + (ngy - 1 - gy) + (nta - 1 - ta)

    @pl.when(later > 0)
    def _():
        pl.semaphore_wait(low_sem.at[0], later)

    greet_line(line_sem.at[0], lines[0])
    tables = [
        weights(h, sizes, (src, disp, mom, perm, phase), (ta, gz), scaling)
        for h in range(lane_rows)
    ]

    def link_at(ref):
        return [
            [
                [jnp.broadcast_to(ref[3 * a + b, pl.ds(part, 1), :].astype(jnp.float32), (8, LANES))
                 for part in range(2)]
                for b in range(3)
            ]
            for a in range(3)
        ]

    wilson = None
    for k in range(1, nsteps + 1):
        if k == 1:
            wilson = link_at(near_links)
        else:
            link_sends[k - 2].wait_recv()
            step = link_at(far_links.at[k - 2])
            wilson = [
                [
                    [
                        sum(wilson[a][c][0] * step[c][b][0] - wilson[a][c][1] * step[c][b][1] for c in range(3)),
                        sum(wilson[a][c][0] * step[c][b][1] + wilson[a][c][1] * step[c][b][0] for c in range(3)),
                    ]
                    for b in range(3)
                ]
                for a in range(3)
            ]
        for chunk in range(size // 16):
            field = [
                [
                    near[part, a, pl.ds(chunk * 16, 16), :].astype(jnp.float32).reshape(2, 8, LANES)
                    for a in range(3)
                ]
                for part in range(2)
            ]
            for b in range(3):
                real = sum(field[0][a] * wilson[a][b][0] + field[1][a] * wilson[a][b][1] for a in range(3))
                imag = sum(field[1][a] * wilson[a][b][0] - field[0][a] * wilson[a][b][1] for a in range(3))
                real, imag = real.reshape(16, LANES), imag.reshape(16, LANES)
                at = 2 * size * b + chunk * 16
                left[pl.ds(at, 16), :] = real
                left[pl.ds(at + size, 16), :] = imag
                turned[pl.ds(at, 16), :] = -imag
                turned[pl.ds(at + size, 16), :] = real
        if k == nsteps:
            pl.semaphore_wait(line_sem.at[0], ngz - 1)
            greet_line(plane_sem.at[0], lines[2])
        sums = None
        for c in range(3):
            sends[k - 1][c].wait_recv()
            keep(right, None, 2 * size * c, size,
                 far[k - 1, 0, c].astype(jnp.float32), far[k - 1, 1, c].astype(jnp.float32))
            sums = add_pairs(sums, left, turned, right, 2 * size * c, 2 * size)
        totals.append(site_sums(sums))

    for h in range(lane_rows):
        table, reach = tables[h]
        chosen = jnp.zeros(table.shape, jnp.float32)
        for k in range(nsteps + 1):
            chosen = jnp.where(reach == k, totals[k], chosen)
        gathered[place, pl.ds(h, 1), :] = jnp.sum(chosen * table, axis=0, keepdims=True)

    def give(at):
        pltpu.make_async_remote_copy(
            src_ref=gathered.at[place], dst_ref=gathered.at[place], send_sem=a_send.at[0],
            recv_sem=a_recv.at[0], device_id=at, device_id_type=MESH).start()

    for root in range(nroots):
        @pl.when(place != root * ngy)
        def _():
            give((0, root, 0))
    pl.semaphore_wait(plane_sem.at[0], nta - 1)
    each(ranks, place, nroots, give)
    others = gathered.at[pl.ds(0, count - 1)]
    pltpu.make_async_copy(others, others, a_recv.at[0]).wait()
    for t in range(nta):
        block = gathered[pl.ds(t * ngz * ngy, ngz * ngy)]
        out[t] = jnp.sum(block, axis=0)
    for copy in link_sends:
        copy.wait_send()
    pltpu.make_async_copy(far, far, s_send.at[0]).wait()
    pltpu.make_async_copy(others, others, a_send.at[0]).wait()


def each(ranks, place, start, act):
    nta, ngz, ngy = ranks
    count = nta * ngz * ngy

    def one(step, along):
        beside = step // (nta * ngz)
        across = step // ngz % nta

        @pl.when(place != (across * ngz + along) * ngy + beside)
        def _():
            act((across, along, beside))

    if count > 64:
        lax.fori_loop(start, count, lambda step, carry: (one(step, step % ngz), carry)[1], 0)
        return
    for step in range(start, count):
        one(step, step % ngz)


def body(ranks, propagator, links, source_z, displacements, momenta, gamma_perm, gamma_phase):
    nta, ngz, ngy = ranks
    sites = propagator.shape[6]
    ndisp, np_, ng = displacements.shape[0], momenta.shape[0], gamma_perm.shape[0]
    nsteps = (ndisp - 1) // 2
    sizes = (ndisp, ng, np_, ngz)
    scaling = 1.0 / (24.0 * math.sqrt(sites * ngy * ngz))
    field = jnp.transpose(propagator, (0, 2, 3, 4, 5, 1, 6)).reshape(2, 3, -1, sites)
    link = jnp.transpose(links, (1, 2, 3, 4, 0, 5)).reshape(9, 2, sites)
    size = field.shape[2]
    regular = pltpu.SemaphoreType.REGULAR
    lane_rows = -(-ndisp * ng * np_ * 2 // LANES)
    more = max(nsteps - 1, 1)
    dma = pltpu.SemaphoreType.DMA
    reduced = pl.pallas_call(
        functools.partial(kernel, sizes, scaling, ranks),
        out_shape=pltpu.VMEM((nta, lane_rows, LANES), jnp.float32),
        in_specs=[pl.BlockSpec(memory_space=pltpu.HBM)] * 7,
        out_specs=pl.BlockSpec(memory_space=pltpu.VMEM),
        scratch_shapes=[
            pltpu.VMEM((2, 3, size, sites), jnp.bfloat16),
            pltpu.VMEM((9, 2, sites), jnp.bfloat16),
            pltpu.VMEM((nsteps, 2, 3, size, sites), jnp.bfloat16),
            pltpu.VMEM((more, 9, 2, sites), jnp.bfloat16),
            pltpu.VMEM((6 * size, sites), jnp.float32),
            pltpu.VMEM((6 * size, sites), jnp.float32),
            pltpu.VMEM((6 * size, sites), jnp.float32),
            pltpu.SMEM(source_z.shape, jnp.int32),
            pltpu.SMEM(displacements.shape, jnp.int32),
            pltpu.SMEM(momenta.shape, jnp.int32),
            pltpu.SMEM(gamma_perm.shape, jnp.int32),
            pltpu.SMEM(gamma_phase.shape, jnp.int32),
            pltpu.VMEM((nta * ngz * ngy, lane_rows, LANES), jnp.float32),
            dma((7,)), dma((1,)), dma((nsteps, 3)),
            dma((1,)), dma((1,)), regular((1,)), regular((1,)), regular((1,)),
        ] + [dma((nsteps - 1,))] * (2 if nsteps > 1 else 0),
        compiler_params=pltpu.CompilerParams(collective_id=0, has_side_effects=True),
    )(field, link, source_z, displacements, momenta, gamma_perm, gamma_phase)
    used = reduced.reshape(nta, lane_rows * LANES)[:, : ndisp * ng * np_ * 2]
    return jnp.swapaxes(used.reshape(nta, ndisp, ng, 2, np_), 3, 4)


def solution(mesh):
    placed = (
        P(None, None, None, None, "ta", "gz", "gy"),
        P(None, None, None, "ta", "gz", "gy"),
        P(),
        P(),
        P(),
        P(),
        P(),
    )
    ranks = tuple(mesh.shape[axis] for axis in ("ta", "gz", "gy"))
    return jax.shard_map(
        functools.partial(body, ranks), mesh=mesh, in_specs=placed, out_specs=P(), check_vma=False
    )
```

```python
import functools
import math

import jax
import jax.numpy as jnp
from jax import lax
from jax.experimental import pallas as pl
from jax.experimental.pallas import tpu as pltpu
from jax.sharding import PartitionSpec as P

MESH = pl.DeviceIdType.MESH
LANES = 128


def weights(lane_row, sizes, smem, place, scaling):
    ndisp, ng, np_, nz = sizes
    src, disp, mom, perm, phase = smem
    slice_at, depth_at = place
    nsteps = (ndisp - 1) // 2
    shape = (32, LANES)
    lane = lax.broadcasted_iota(jnp.int32, shape, 1)
    momentum = lane & (np_ - 1)
    lane = lane_row * LANES + LANES - np_ - (lane - momentum)
    row = lax.broadcasted_iota(jnp.int32, shape, 0)
    out_part = (lane // np_) & 1
    gamma = (lane // (2 * np_)) & (ng - 1)
    entry = lane // (2 * np_ * ng)
    in_part = row // 16
    first = (row // 4) & 3
    second = row & 3
    reach = jnp.full(shape, 2 * nsteps + 1, jnp.int32)
    for j in range(ndisp):
        reach = jnp.where(entry == j, disp[j] - nsteps, reach)
    backward = reach < 0
    momenta = jnp.zeros(shape, jnp.int32)
    source = jnp.zeros(shape, jnp.int32)
    for p in range(np_):
        momenta = jnp.where(momentum == p, mom[p], momenta)
        source = jnp.where(momentum == p, src[slice_at, p], source)
    depth = depth_at - jnp.where(backward, reach, 0)
    turns = (momenta * (depth - source)).astype(jnp.float32) * (1.0 / nz)
    angle = (turns - jnp.floor(turns)) * (2.0 * math.pi)
    cosine = jnp.cos(angle)
    sine = jnp.sin(angle)
    sink = jnp.where(backward, second, first)
    other = jnp.where(backward, first, second)
    column = jnp.zeros(shape, jnp.int32)
    power = jnp.zeros(shape, jnp.int32)
    for g in range(ng):
        for s in range(4):
            here = (gamma == g) & (sink == s)
            column = jnp.where(here, perm[g, s], column)
            power = jnp.where(here, phase[g, s], power)
    quarter = power - out_part + jnp.where(backward, -in_part, in_part)
    quarter = quarter & 3
    value = jnp.where((quarter & 1) == 0, cosine, sine)
    value = jnp.where(quarter >= 2, -value, value)
    value = jnp.where((column == other) & (entry < ndisp), value * scaling, 0.0)
    return value, jnp.abs(reach)


def add_pairs(sums, left, turned, right, start, size):
    def rows(ref, s):
        return ref[pl.ds(start + s, size // 4, stride=4), :].reshape(-1, 8, LANES)

    rights = [rows(right, u) for u in range(4)]
    out = []
    for side in (left, turned):
        for s in range(4):
            own = rows(side, s)
            out += [jnp.sum(own * other, axis=0) for other in rights]
    return out if sums is None else [x + y for x, y in zip(sums, out)]


def site_sums(sums):
    stacked = jnp.concatenate([jnp.sum(x, axis=0, keepdims=True) for x in sums], axis=0)
    return jnp.sum(stacked, axis=1, keepdims=True)


def keep(left, turned, at, size, real, imag):
    real, imag = real.reshape(-1, LANES), imag.reshape(-1, LANES)
    left[pl.ds(at, size), :] = real
    left[pl.ds(at + size, size), :] = imag
    if turned is not None:
        turned[pl.ds(at, size), :] = -imag
        turned[pl.ds(at + size, size), :] = real


def kernel(
    sizes, scaling, ranks,
    prop, links, src_h, disp_h, mom_h, perm_h, phase_h,
    out,
    near, near_links, far, far_links, left, turned, right,
    src, disp, mom, perm, phase,
    gathered,
    local_sem, s_send, s_recv, a_recv, low_sem, line_sem, plane_sem, *link_sems,
):
    ndisp, ng, np_, nz = sizes
    nta, ngz, ngy = ranks
    nsteps = (ndisp - 1) // 2
    size = near.shape[2]
    lane_rows = gathered.shape[1]
    ta, gz, gy = lax.axis_index("ta"), lax.axis_index("gz"), lax.axis_index("gy")
    place = (ta * ngz + gz) * ngy + gy

    loads = [
        pltpu.make_async_copy(a, b, local_sem.at[i])
        for i, (a, b) in enumerate(
            [(prop.at[:, c], near.at[:, c]) for c in range(3)] + [(links, near_links)]
        )
    ]
    smalls = [
        pltpu.make_async_copy(a, b, local_sem.at[i])
        for i, (a, b) in enumerate(
            [(src_h, src), (disp_h, disp), (mom_h, mom), (perm_h, perm), (phase_h, phase)]
        )
    ]

    lines = [
        (gz, ngz, lambda i: (ta, i, gy)),
        (gy, ngy, lambda i: (ta, gz, i)),
        (ta, nta, lambda i: (i, gz, gy)),
    ]

    def greet(semaphore, at):
        pl.semaphore_signal(semaphore, inc=1, device_id=at, device_id_type=MESH)

    def greet_span(semaphore, line, low, high):
        lax.fori_loop(low, high, lambda i, carry: (greet(semaphore, line[2](i)), carry)[1], 0)

    def greet_line(semaphore, line):
        greet_span(semaphore, line, 0, line[0])
        greet_span(semaphore, line, line[0] + 1, line[1])

    count = nta * ngz * ngy
    barrier = pltpu.get_barrier_semaphore()
    for k in range(1, nsteps + 1):
        @pl.when(gz + k >= ngz)
        def _():
            greet(barrier, (ta, gz + k - ngz, gy))
    for load in loads:
        load.start()
    for line in lines:
        greet_span(barrier, line, line[0] + 1, line[1])
    nroots = min(2, ngz)
    is_root = (ta + gy == 0) & (gz < nroots)

    @pl.when(is_root)
    def _():
        def one(step, carry):
            at = (step // (ngz * ngy), step // ngy % ngz, step % ngy)

            @pl.when(step != place)
            def _():
                greet(barrier, at)

            return carry

        lax.fori_loop(0, count, one, 0)

    pl.semaphore_wait(
        barrier,
        jnp.maximum(gz, nsteps) + gy + ta + nroots - jnp.where(is_root, 1, 0),
    )

    def target(k):
        return (ta, lax.rem(gz + ngz - k, ngz), gy)

    sends = [
        [
            pltpu.make_async_remote_copy(
                src_ref=near.at[:, c], dst_ref=far.at[k - 1, :, c], send_sem=s_send.at[0],
                recv_sem=s_recv.at[k - 1, c], device_id=target(k), device_id_type=MESH)
            for c in range(3)
        ]
        for k in range(1, nsteps + 1)
    ]
    u_send, u_recv = link_sems if link_sems else (None, None)
    link_sends = [
        pltpu.make_async_remote_copy(
            src_ref=near_links, dst_ref=far_links.at[k - 1], send_sem=u_send.at[k - 1],
            recv_sem=u_recv.at[k - 1], device_id=target(k), device_id_type=MESH)
        for k in range(1, nsteps)
    ]
    for c in range(3):
        loads[c].wait()
        for copies in sends:
            copies[c].start()
    for line in lines:
        greet_span(low_sem.at[0], line, 0, line[0])
    loads[3].wait()
    for small in smalls:
        small.start()
    for copy in link_sends:
        copy.start()
    sums = None
    for c in range(3):
        keep(left, turned, 2 * size * c, size, near[0, c].astype(jnp.float32), near[1, c].astype(jnp.float32))
        sums = add_pairs(sums, left, turned, left, 2 * size * c, 2 * size)
    totals = [site_sums(sums)]
    for small in smalls:
        small.wait()
    later = (ngz - 1 - gz) + (ngy - 1 - gy) + (nta - 1 - ta)
    inner = lax.rem(gz, 2) == 0

    def meet_depth():
        @pl.when(later > 0)
        def _():
            pl.semaphore_wait(low_sem.at[0], later)

        greet_line(line_sem.at[0], lines[0])

    def meet_across():
        pl.semaphore_wait(line_sem.at[0], ngz - 1)
        greet_line(plane_sem.at[0], lines[2])

    pl.when(jnp.logical_not(inner))(meet_depth)
    tables = [
        weights(h, sizes, (src, disp, mom, perm, phase), (ta, gz), scaling)
        for h in range(lane_rows)
    ]

    def link_at(ref):
        return [
            [
                [jnp.broadcast_to(ref[3 * a + b, pl.ds(part, 1), :].astype(jnp.float32), (8, LANES))
                 for part in range(2)]
                for b in range(3)
            ]
            for a in range(3)
        ]

    wilson = None
    for k in range(1, nsteps + 1):
        if k == 1:
            wilson = link_at(near_links)
        else:
            link_sends[k - 2].wait_recv()
            step = link_at(far_links.at[k - 2])
            wilson = [
                [
                    [
                        sum(wilson[a][c][0] * step[c][b][0] - wilson[a][c][1] * step[c][b][1] for c in range(3)),
                        sum(wilson[a][c][0] * step[c][b][1] + wilson[a][c][1] * step[c][b][0] for c in range(3)),
                    ]
                    for b in range(3)
                ]
                for a in range(3)
            ]
        for chunk in range(size // 16):
            field = [
                [
                    near[part, a, pl.ds(chunk * 16, 16), :].astype(jnp.float32).reshape(2, 8, LANES)
                    for a in range(3)
                ]
                for part in range(2)
            ]
            for b in range(3):
                real = sum(field[0][a] * wilson[a][b][0] + field[1][a] * wilson[a][b][1] for a in range(3))
                imag = sum(field[1][a] * wilson[a][b][0] - field[0][a] * wilson[a][b][1] for a in range(3))
                real, imag = real.reshape(16, LANES), imag.reshape(16, LANES)
                at = 2 * size * b + chunk * 16
                left[pl.ds(at, 16), :] = real
                left[pl.ds(at + size, 16), :] = imag
                turned[pl.ds(at, 16), :] = -imag
                turned[pl.ds(at + size, 16), :] = real
        sums = None
        for c in range(3):
            if k == nsteps and c == 2:
                pl.when(jnp.logical_not(inner))(meet_across)
            sends[k - 1][c].wait_recv()
            keep(right, None, 2 * size * c, size,
                 far[k - 1, 0, c].astype(jnp.float32), far[k - 1, 1, c].astype(jnp.float32))
            sums = add_pairs(sums, left, turned, right, 2 * size * c, 2 * size)
        totals.append(site_sums(sums))

    for h in range(lane_rows):
        table, reach = tables[h]
        chosen = jnp.zeros(table.shape, jnp.float32)
        for k in range(nsteps + 1):
            chosen = jnp.where(reach == k, totals[k], chosen)
        gathered[place, pl.ds(h, 1), :] = jnp.sum(chosen * table, axis=0, keepdims=True)

    def give(at):
        pltpu.make_async_remote_copy(
            src_ref=gathered.at[place], dst_ref=gathered.at[place], send_sem=s_send.at[0],
            recv_sem=a_recv.at[0], device_id=at, device_id_type=MESH).start()

    for root in range(nroots):
        @pl.when(place != root * ngy)
        def _():
            give((0, root, 0))
    @pl.when(inner)
    def _():
        meet_depth()
        meet_across()

    pl.semaphore_wait(plane_sem.at[0], nta - 1)
    each(ranks, place, nroots, give)
    others = gathered.at[pl.ds(0, count - 1)]
    pltpu.make_async_copy(others, others, a_recv.at[0]).wait()
    for t in range(nta):
        for h in range(lane_rows):
            total = row_sum(gathered, t * ngz * ngy, ngz * ngy, h)
            low = h * (LANES // np_)
            for row in range(low, min(low + LANES // np_, out.shape[1]), 8):
                shift = (1 + row - low) * np_
                out[t, pl.ds(row, 8), :] = pltpu.roll(total, shift, 1, stride=np_, stride_axis=0)[:, :np_]
    for copy in link_sends:
        copy.wait_send()
    pltpu.make_async_copy(far, far, s_send.at[0]).wait()
    pltpu.make_async_copy(others, others, s_send.at[0]).wait()


def row_sum(ref, start, size, h):
    if size > 32:
        total = jnp.sum(ref[pl.ds(start, size), pl.ds(h, 1), :], axis=0)
        return jnp.broadcast_to(total, (8, LANES))
    terms = [jnp.broadcast_to(ref[start + i, pl.ds(h, 1), :], (8, LANES)) for i in range(size)]
    while len(terms) > 1:
        terms = [sum(terms[i:i + 2]) for i in range(0, len(terms), 2)]
    return terms[0]


def each(ranks, place, start, act):
    nta, ngz, ngy = ranks
    count = nta * ngz * ngy

    def one(step, along):
        beside = step // (nta * ngz)
        across = step // ngz % nta

        @pl.when(place != (across * ngz + along) * ngy + beside)
        def _():
            act((across, along, beside))

    if count > 64:
        lax.fori_loop(start, count, lambda step, carry: (one(step, step % ngz), carry)[1], 0)
        return
    for step in range(start, count):
        one(step, step % ngz)


def body(ranks, propagator, links, source_z, displacements, momenta, gamma_perm, gamma_phase):
    nta, ngz, ngy = ranks
    sites = propagator.shape[6]
    ndisp, np_, ng = displacements.shape[0], momenta.shape[0], gamma_perm.shape[0]
    nsteps = (ndisp - 1) // 2
    sizes = (ndisp, ng, np_, ngz)
    scaling = 1.0 / (24.0 * math.sqrt(sites * ngy * ngz))
    field = jnp.transpose(propagator, (0, 2, 3, 4, 5, 1, 6)).reshape(2, 3, -1, sites)
    link = jnp.transpose(links, (1, 2, 3, 4, 0, 5)).reshape(9, 2, sites)
    size = field.shape[2]
    regular = pltpu.SemaphoreType.REGULAR
    lane_rows = -(-ndisp * ng * np_ * 2 // LANES)
    more = max(nsteps - 1, 1)
    dma = pltpu.SemaphoreType.DMA
    reduced = pl.pallas_call(
        functools.partial(kernel, sizes, scaling, ranks),
        out_shape=pltpu.VMEM((nta, ndisp * ng * 2, np_), jnp.float32),
        in_specs=[pl.BlockSpec(memory_space=pltpu.HBM)] * 7,
        out_specs=pl.BlockSpec(memory_space=pltpu.VMEM),
        scratch_shapes=[
            pltpu.VMEM((2, 3, size, sites), jnp.bfloat16),
            pltpu.VMEM((9, 2, sites), jnp.bfloat16),
            pltpu.VMEM((nsteps, 2, 3, size, sites), jnp.bfloat16),
            pltpu.VMEM((more, 9, 2, sites), jnp.bfloat16),
            pltpu.VMEM((6 * size, sites), jnp.float32),
            pltpu.VMEM((6 * size, sites), jnp.float32),
            pltpu.VMEM((6 * size, sites), jnp.float32),
            pltpu.SMEM(source_z.shape, jnp.int32),
            pltpu.SMEM(displacements.shape, jnp.int32),
            pltpu.SMEM(momenta.shape, jnp.int32),
            pltpu.SMEM(gamma_perm.shape, jnp.int32),
            pltpu.SMEM(gamma_phase.shape, jnp.int32),
            pltpu.VMEM((nta * ngz * ngy, lane_rows, LANES), jnp.float32),
            dma((5,)), dma((1,)), dma((nsteps, 3)),
            dma((1,)), regular((1,)), regular((1,)), regular((1,)),
        ] + [dma((nsteps - 1,))] * (2 if nsteps > 1 else 0),
        compiler_params=pltpu.CompilerParams(collective_id=0, has_side_effects=True),
    )(field, link, source_z, displacements, momenta, gamma_perm, gamma_phase)
    return jnp.swapaxes(reduced.reshape(nta, ndisp, ng, 2, np_), 3, 4)


def solution(mesh):
    placed = (
        P(None, None, None, None, "ta", "gz", "gy"),
        P(None, None, None, "ta", "gz", "gy"),
        P(),
        P(),
        P(),
        P(),
        P(),
    )
    ranks = tuple(mesh.shape[axis] for axis in ("ta", "gz", "gy"))
    return jax.shard_map(
        functools.partial(body, ranks), mesh=mesh, in_specs=placed, out_specs=P(), check_vma=False
    )
```

```python
import functools
import math

import jax
import jax.numpy as jnp
from jax import lax
from jax.experimental import pallas as pl
from jax.experimental.pallas import tpu as pltpu
from jax.sharding import PartitionSpec as P

MESH = pl.DeviceIdType.MESH
LANES = 128


def weights(lane_row, sizes, smem, place, scaling):
    ndisp, ng, np_, nz = sizes
    src, disp, mom, perm, phase = smem
    slice_at, depth_at = place
    nsteps = (ndisp - 1) // 2
    shape = (32, LANES)
    lane = lax.broadcasted_iota(jnp.int32, shape, 1)
    momentum = lane & (np_ - 1)
    lane = lane_row * LANES + LANES - np_ - (lane - momentum)
    row = lax.broadcasted_iota(jnp.int32, shape, 0)
    out_part = (lane // np_) & 1
    gamma = (lane // (2 * np_)) & (ng - 1)
    entry = lane // (2 * np_ * ng)
    in_part = row // 16
    first = (row // 4) & 3
    second = row & 3
    reach = jnp.full(shape, 2 * nsteps + 1, jnp.int32)
    for j in range(ndisp):
        reach = jnp.where(entry == j, disp[j] - nsteps, reach)
    backward = reach < 0
    momenta = jnp.zeros(shape, jnp.int32)
    source = jnp.zeros(shape, jnp.int32)
    for p in range(np_):
        momenta = jnp.where(momentum == p, mom[p], momenta)
        source = jnp.where(momentum == p, src[slice_at, p], source)
    depth = depth_at - jnp.where(backward, reach, 0)
    turns = (momenta * (depth - source)).astype(jnp.float32) * (1.0 / nz)
    angle = (turns - jnp.floor(turns)) * (2.0 * math.pi)
    cosine = jnp.cos(angle)
    sine = jnp.sin(angle)
    sink = jnp.where(backward, second, first)
    other = jnp.where(backward, first, second)
    column = jnp.zeros(shape, jnp.int32)
    power = jnp.zeros(shape, jnp.int32)
    for g in range(ng):
        for s in range(4):
            here = (gamma == g) & (sink == s)
            column = jnp.where(here, perm[g, s], column)
            power = jnp.where(here, phase[g, s], power)
    quarter = power - out_part + jnp.where(backward, -in_part, in_part)
    quarter = quarter & 3
    value = jnp.where((quarter & 1) == 0, cosine, sine)
    value = jnp.where(quarter >= 2, -value, value)
    value = jnp.where((column == other) & (entry < ndisp), value * scaling, 0.0)
    return value, jnp.abs(reach)


def add_pairs(sums, left, turned, right, start, size):
    def rows(ref, s):
        return ref[pl.ds(start + s, size // 4, stride=4), :].reshape(-1, 8, LANES)

    rights = [rows(right, u) for u in range(4)]
    out = []
    for side in (left, turned):
        for s in range(4):
            own = rows(side, s)
            out += [jnp.sum(own * other, axis=0) for other in rights]
    return out if sums is None else [x + y for x, y in zip(sums, out)]


def site_sums(sums):
    stacked = jnp.concatenate([jnp.sum(x, axis=0, keepdims=True) for x in sums], axis=0)
    return jnp.sum(stacked, axis=1, keepdims=True)


def keep(left, turned, at, size, real, imag):
    real, imag = real.reshape(-1, LANES), imag.reshape(-1, LANES)
    left[pl.ds(at, size), :] = real
    left[pl.ds(at + size, size), :] = imag
    if turned is not None:
        turned[pl.ds(at, size), :] = -imag
        turned[pl.ds(at + size, size), :] = real


def self_sums(field, left, turned, size):
    sums = None
    for c in range(3):
        keep(left, turned, 2 * size * c, size, field[0, c].astype(jnp.float32), field[1, c].astype(jnp.float32))
        sums = add_pairs(sums, left, turned, left, 2 * size * c, 2 * size)
    return site_sums(sums)


def link_at(ref):
    return [
        [
            [jnp.broadcast_to(ref[3 * a + b, pl.ds(part, 1), :].astype(jnp.float32), (8, LANES))
             for part in range(2)]
            for b in range(3)
        ]
        for a in range(3)
    ]


def carry_link(near, wilson, left, turned, size):
    for chunk in range(size // 16):
        field = [
            [
                near[part, a, pl.ds(chunk * 16, 16), :].astype(jnp.float32).reshape(2, 8, LANES)
                for a in range(3)
            ]
            for part in range(2)
        ]
        for b in range(3):
            real = sum(field[0][a] * wilson[a][b][0] + field[1][a] * wilson[a][b][1] for a in range(3))
            imag = sum(field[1][a] * wilson[a][b][0] - field[0][a] * wilson[a][b][1] for a in range(3))
            real, imag = real.reshape(16, LANES), imag.reshape(16, LANES)
            at = 2 * size * b + chunk * 16
            left[pl.ds(at, 16), :] = real
            left[pl.ds(at + size, 16), :] = imag
            turned[pl.ds(at, 16), :] = -imag
            turned[pl.ds(at + size, 16), :] = real


def pair_sums(far, left, turned, right, size, before):
    sums = None
    for c in range(3):
        before(c)
        keep(right, None, 2 * size * c, size, far[0, c].astype(jnp.float32), far[1, c].astype(jnp.float32))
        sums = add_pairs(sums, left, turned, right, 2 * size * c, 2 * size)
    return site_sums(sums)


def row_of(totals, table, reach):
    chosen = jnp.zeros(table.shape, jnp.float32)
    for k, total in enumerate(totals):
        chosen = jnp.where(reach == k, total, chosen)
    return jnp.sum(chosen * table, axis=0, keepdims=True)


def kernel(sizes, scaling, ranks, helped, *refs):
    refs = list(refs)
    prop, links, src_h, disp_h, mom_h, perm_h, phase_h, out = refs[:8]
    near, near_links, far, far_links, left, turned, right = refs[8:15]
    rest = refs[15:]
    heap = heap_links = heap_left = heap_turned = heap_tables = None
    if helped:
        heap, heap_links, heap_left, heap_turned, heap_tables = rest[:5]
        rest = rest[5:]
    src, disp, mom, perm, phase, gathered = rest[:6]
    local_sem, s_send, s_recv, a_recv, low_sem, line_sem, plane_sem = rest[6:13]
    rest = rest[13:]
    heap_recv = heap_links_recv = None
    if helped:
        heap_recv, heap_links_recv = rest[:2]
        rest = rest[2:]
    link_sems = rest
    ndisp, ng, np_, nz = sizes
    nta, ngz, ngy = ranks
    nsteps = (ndisp - 1) // 2
    size = near.shape[2]
    lane_rows = gathered.shape[1]
    ta, gz, gy = lax.axis_index("ta"), lax.axis_index("gz"), lax.axis_index("gy")
    place = (ta * ngz + gz) * ngy + gy

    loads = [
        pltpu.make_async_copy(a, b, local_sem.at[i])
        for i, (a, b) in enumerate(
            [(prop.at[:, c], near.at[:, c]) for c in range(3)] + [(links, near_links)]
        )
    ]
    smalls = [
        pltpu.make_async_copy(a, b, local_sem.at[i])
        for i, (a, b) in enumerate(
            [(src_h, src), (disp_h, disp), (mom_h, mom), (perm_h, perm), (phase_h, phase)]
        )
    ]

    lines = [
        (gz, ngz, lambda i: (ta, i, gy)),
        (gy, ngy, lambda i: (ta, gz, i)),
        (ta, nta, lambda i: (i, gz, gy)),
    ]

    def greet(semaphore, at):
        pl.semaphore_signal(semaphore, inc=1, device_id=at, device_id_type=MESH)

    def greet_span(semaphore, line, low, high):
        lax.fori_loop(low, high, lambda i, carry: (greet(semaphore, line[2](i)), carry)[1], 0)

    def greet_line(semaphore, line):
        greet_span(semaphore, line, 0, line[0])
        greet_span(semaphore, line, line[0] + 1, line[1])

    count = nta * ngz * ngy
    barrier = pltpu.get_barrier_semaphore()
    for k in range(1, nsteps + 1):
        @pl.when(gz + k >= ngz)
        def _():
            greet(barrier, (ta, gz + k - ngz, gy))
    for load in loads:
        load.start()
    for line in lines:
        greet_span(barrier, line, line[0] + 1, line[1])
    nroots = min(2, ngz)
    is_root = (ta + gy == 0) & (gz < nroots)
    helper_at = (0, nroots - 1, 0)
    is_helper = (ta + gy == 0) & (gz == nroots - 1)
    is_distant = (ta == nta - 1) & (gy == ngy - 1)
    is_served = is_distant & (lax.rem(gz, 2) == 1)
    served = list(range(1, ngz, 2)) if helped else []

    def place_of(z):
        return ((nta - 1) * ngz + z) * ngy + ngy - 1

    @pl.when(is_root)
    def _():
        def one(step, carry):
            at = (step // (ngz * ngy), step // ngy % ngz, step % ngy)

            @pl.when(step != place)
            def _():
                greet(barrier, at)

            return carry

        lax.fori_loop(0, count, one, 0)

    pl.semaphore_wait(
        barrier,
        jnp.maximum(gz, nsteps) + gy + ta + nroots - jnp.where(is_root, 1, 0),
    )

    def target(k):
        return (ta, lax.rem(gz + ngz - k, ngz), gy)

    sends = [
        [
            pltpu.make_async_remote_copy(
                src_ref=near.at[:, c], dst_ref=far.at[k - 1, :, c], send_sem=s_send.at[0],
                recv_sem=s_recv.at[k - 1, c], device_id=target(k), device_id_type=MESH)
            for c in range(3)
        ]
        for k in range(1, nsteps + 1)
    ]
    u_send, u_recv = link_sems if link_sems else (None, None)
    link_sends = [
        pltpu.make_async_remote_copy(
            src_ref=near_links, dst_ref=far_links.at[k - 1], send_sem=u_send.at[k - 1],
            recv_sem=u_recv.at[k - 1], device_id=target(k), device_id_type=MESH)
        for k in range(1, nsteps)
    ]
    for c in range(3):
        loads[c].wait()
        for copies in sends:
            copies[c].start()
    for line in lines:
        greet_span(low_sem.at[0], line, 0, line[0])
    loads[3].wait()
    if helped:
        @pl.when(is_distant)
        def _():
            pltpu.make_async_remote_copy(
                src_ref=near, dst_ref=heap.at[gz], send_sem=s_send.at[0], recv_sem=heap_recv.at[gz],
                device_id=helper_at, device_id_type=MESH).start()

        @pl.when(is_served)
        def _():
            pltpu.make_async_remote_copy(
                src_ref=near_links, dst_ref=heap_links.at[gz // 2], send_sem=s_send.at[0],
                recv_sem=heap_links_recv.at[gz // 2], device_id=helper_at, device_id_type=MESH).start()
    for small in smalls:
        small.start()
    for copy in link_sends:
        copy.start()
    totals = [self_sums(near, left, turned, size)]
    for small in smalls:
        small.wait()
    later = (ngz - 1 - gz) + (ngy - 1 - gy) + (nta - 1 - ta)
    inner = lax.rem(gz, 2) == 0

    def meet_depth():
        @pl.when(later > 0)
        def _():
            pl.semaphore_wait(low_sem.at[0], later)

        greet_line(line_sem.at[0], lines[0])

    def meet_across():
        pl.semaphore_wait(line_sem.at[0], ngz - 1)
        greet_line(plane_sem.at[0], lines[2])

    pl.when(jnp.logical_not(inner))(meet_depth)
    tables = [
        weights(h, sizes, (src, disp, mom, perm, phase), (ta, gz), scaling)
        for h in range(lane_rows)
    ]

    if helped:
        @pl.when(is_helper)
        def _():
            for z in served:
                for h in range(lane_rows):
                    heap_tables[z // 2, h] = weights(
                        h, sizes, (src, disp, mom, perm, phase), (nta - 1, z), scaling)[0]

    wilson = None
    for k in range(1, nsteps + 1):
        if k == 1:
            wilson = link_at(near_links)
        else:
            link_sends[k - 2].wait_recv()
            step = link_at(far_links.at[k - 2])
            wilson = [
                [
                    [
                        sum(wilson[a][c][0] * step[c][b][0] - wilson[a][c][1] * step[c][b][1] for c in range(3)),
                        sum(wilson[a][c][0] * step[c][b][1] + wilson[a][c][1] * step[c][b][0] for c in range(3)),
                    ]
                    for b in range(3)
                ]
                for a in range(3)
            ]
        carry_link(near, wilson, left, turned, size)

        def before(c):
            if k == nsteps and c == 2:
                pl.when(jnp.logical_not(inner))(meet_across)
            sends[k - 1][c].wait_recv()

        totals.append(pair_sums(far.at[k - 1], left, turned, right, size, before))

    for h in range(lane_rows):
        gathered[place, pl.ds(h, 1), :] = row_of(totals, *tables[h])

    def give(at, row=place):
        pltpu.make_async_remote_copy(
            src_ref=gathered.at[row], dst_ref=gathered.at[row], send_sem=s_send.at[0],
            recv_sem=a_recv.at[0], device_id=at, device_id_type=MESH).start()

    for root in range(nroots):
        @pl.when((place != root * ngy) & jnp.logical_not(is_served & helped))
        def _():
            give((0, root, 0))
    @pl.when(inner)
    def _():
        meet_depth()
        meet_across()

    pl.semaphore_wait(plane_sem.at[0], nta - 1)
    each(ranks, place, nroots, give)
    if helped:
        @pl.when(is_helper)
        def _():
            first = []
            for z in served:
                slot = z // 2
                pltpu.make_async_copy(heap.at[z], heap.at[z], heap_recv.at[z]).wait()
                pltpu.make_async_copy(heap_links.at[slot], heap_links.at[slot], heap_links_recv.at[slot]).wait()
                first.append(self_sums(heap.at[z], heap_left.at[slot], heap_turned.at[slot], size))
                carry_link(heap.at[z], link_at(heap_links.at[slot]), heap_left.at[slot], heap_turned.at[slot], size)
            for z in reversed(served):
                slot, other = z // 2, (z + 1) % ngz
                pltpu.make_async_copy(heap.at[other], heap.at[other], heap_recv.at[other]).wait()
                pair = pair_sums(
                    heap.at[other], heap_left.at[slot], heap_turned.at[slot], right, size, lambda c: None)
                for h in range(lane_rows):
                    gathered[place_of(z), pl.ds(h, 1), :] = row_of(
                        [first[slot], pair], heap_tables[slot, h], tables[h][1])
                for root in range(nroots - 1):
                    give((0, root, 0), place_of(z))

    def rows_done(semaphore, rows):
        if rows > 0:
            pltpu.make_async_copy(gathered.at[pl.ds(0, rows)], gathered.at[pl.ds(0, rows)], semaphore).wait()

    mine = len(served)
    if helped:
        pl.when(is_helper)(lambda: rows_done(a_recv.at[0], count - 1 - mine))
        pl.when(jnp.logical_not(is_helper))(lambda: rows_done(a_recv.at[0], count - 1))
    else:
        rows_done(a_recv.at[0], count - 1)
    for t in range(nta):
        for h in range(lane_rows):
            total = row_sum(gathered, t * ngz * ngy, ngz * ngy, h)
            low = h * (LANES // np_)
            for row in range(low, min(low + LANES // np_, out.shape[1]), 8):
                shift = (1 + row - low) * np_
                out[t, pl.ds(row, 8), :] = pltpu.roll(total, shift, 1, stride=np_, stride_axis=0)[:, :np_]
    for copy in link_sends:
        copy.wait_send()
    pltpu.make_async_copy(far, far, s_send.at[0]).wait()
    if helped:
        @pl.when(is_distant)
        def _():
            pltpu.make_async_copy(near, near, s_send.at[0]).wait()

        @pl.when(is_served)
        def _():
            pltpu.make_async_copy(near_links, near_links, s_send.at[0]).wait()

        pl.when(is_helper)(lambda: rows_done(s_send.at[0], mine * (nroots - 1)))
        pl.when(jnp.logical_not(is_served))(lambda: rows_done(s_send.at[0], nroots))
        rows_done(s_send.at[0], count - 1 - nroots)
    else:
        rows_done(s_send.at[0], count - 1)


def row_sum(ref, start, size, h):
    if size > 32:
        total = jnp.sum(ref[pl.ds(start, size), pl.ds(h, 1), :], axis=0)
        return jnp.broadcast_to(total, (8, LANES))
    terms = [jnp.broadcast_to(ref[start + i, pl.ds(h, 1), :], (8, LANES)) for i in range(size)]
    while len(terms) > 1:
        terms = [sum(terms[i:i + 2]) for i in range(0, len(terms), 2)]
    return terms[0]


def each(ranks, place, start, act):
    nta, ngz, ngy = ranks
    count = nta * ngz * ngy

    def one(step, along):
        beside = step // (nta * ngz)
        across = step // ngz % nta

        @pl.when(place != (across * ngz + along) * ngy + beside)
        def _():
            act((across, along, beside))

    if count > 64:
        lax.fori_loop(start, count, lambda step, carry: (one(step, step % ngz), carry)[1], 0)
        return
    for step in range(start, count):
        one(step, step % ngz)


def body(ranks, propagator, links, source_z, displacements, momenta, gamma_perm, gamma_phase):
    nta, ngz, ngy = ranks
    sites = propagator.shape[6]
    ndisp, np_, ng = displacements.shape[0], momenta.shape[0], gamma_perm.shape[0]
    nsteps = (ndisp - 1) // 2
    sizes = (ndisp, ng, np_, ngz)
    scaling = 1.0 / (24.0 * math.sqrt(sites * ngy * ngz))
    field = jnp.transpose(propagator, (0, 2, 3, 4, 5, 1, 6)).reshape(2, 3, -1, sites)
    link = jnp.transpose(links, (1, 2, 3, 4, 0, 5)).reshape(9, 2, sites)
    size = field.shape[2]
    regular = pltpu.SemaphoreType.REGULAR
    lane_rows = -(-ndisp * ng * np_ * 2 // LANES)
    more = max(nsteps - 1, 1)
    dma = pltpu.SemaphoreType.DMA
    helped = nsteps == 1 and ngz == 4 and nta * ngy > 1
    pairs = ngz // 2
    heaps = [
        pltpu.VMEM((ngz, 2, 3, size, sites), jnp.bfloat16),
        pltpu.VMEM((pairs, 9, 2, sites), jnp.bfloat16),
        pltpu.VMEM((pairs, 6 * size, sites), jnp.float32),
        pltpu.VMEM((pairs, 6 * size, sites), jnp.float32),
        pltpu.VMEM((pairs, lane_rows, 32, LANES), jnp.float32),
    ] if helped else []
    heap_sems = [dma((ngz,)), dma((pairs,))] if helped else []
    reduced = pl.pallas_call(
        functools.partial(kernel, sizes, scaling, ranks, helped),
        out_shape=pltpu.VMEM((nta, ndisp * ng * 2, np_), jnp.float32),
        in_specs=[pl.BlockSpec(memory_space=pltpu.HBM)] * 7,
        out_specs=pl.BlockSpec(memory_space=pltpu.VMEM),
        scratch_shapes=[
            pltpu.VMEM((2, 3, size, sites), jnp.bfloat16),
            pltpu.VMEM((9, 2, sites), jnp.bfloat16),
            pltpu.VMEM((nsteps, 2, 3, size, sites), jnp.bfloat16),
            pltpu.VMEM((more, 9, 2, sites), jnp.bfloat16),
            pltpu.VMEM((6 * size, sites), jnp.float32),
            pltpu.VMEM((6 * size, sites), jnp.float32),
            pltpu.VMEM((6 * size, sites), jnp.float32),
            *heaps,
            pltpu.SMEM(source_z.shape, jnp.int32),
            pltpu.SMEM(displacements.shape, jnp.int32),
            pltpu.SMEM(momenta.shape, jnp.int32),
            pltpu.SMEM(gamma_perm.shape, jnp.int32),
            pltpu.SMEM(gamma_phase.shape, jnp.int32),
            pltpu.VMEM((nta * ngz * ngy, lane_rows, LANES), jnp.float32),
            dma((5,)), dma((1,)), dma((nsteps, 3)),
            dma((1,)), regular((1,)), regular((1,)), regular((1,)),
            *heap_sems,
        ] + [dma((nsteps - 1,))] * (2 if nsteps > 1 else 0),
        compiler_params=pltpu.CompilerParams(collective_id=0, has_side_effects=True),
    )(field, link, source_z, displacements, momenta, gamma_perm, gamma_phase)
    return jnp.swapaxes(reduced.reshape(nta, ndisp, ng, 2, np_), 3, 4)


def solution(mesh):
    placed = (
        P(None, None, None, None, "ta", "gz", "gy"),
        P(None, None, None, "ta", "gz", "gy"),
        P(),
        P(),
        P(),
        P(),
        P(),
    )
    ranks = tuple(mesh.shape[axis] for axis in ("ta", "gz", "gy"))
    return jax.shard_map(
        functools.partial(body, ranks), mesh=mesh, in_specs=placed, out_specs=P(), check_vma=False
    )
```

```python
import functools
import math

import jax
import jax.numpy as jnp
from jax import lax
from jax.experimental import pallas as pl
from jax.experimental.pallas import tpu as pltpu
from jax.sharding import PartitionSpec as P

MESH = pl.DeviceIdType.MESH
PIECES = ((0, 2), (2, 1))
LANES = 128


def weights(lane_row, sizes, smem, place, scaling):
    ndisp, ng, np_, nz = sizes
    src, disp, mom, perm, phase = smem
    slice_at, depth_at = place
    nsteps = (ndisp - 1) // 2
    shape = (32, LANES)
    lane = lax.broadcasted_iota(jnp.int32, shape, 1)
    momentum = lane & (np_ - 1)
    lane = lane_row * LANES + LANES - np_ - (lane - momentum)
    row = lax.broadcasted_iota(jnp.int32, shape, 0)
    out_part = (lane // np_) & 1
    gamma = (lane // (2 * np_)) & (ng - 1)
    entry = lane // (2 * np_ * ng)
    in_part = row // 16
    first = (row // 4) & 3
    second = row & 3
    reach = jnp.full(shape, 2 * nsteps + 1, jnp.int32)
    for j in range(ndisp):
        reach = jnp.where(entry == j, disp[j] - nsteps, reach)
    backward = reach < 0
    momenta = jnp.zeros(shape, jnp.int32)
    source = jnp.zeros(shape, jnp.int32)
    for p in range(np_):
        momenta = jnp.where(momentum == p, mom[p], momenta)
        source = jnp.where(momentum == p, src[slice_at, p], source)
    depth = depth_at - jnp.where(backward, reach, 0)
    turns = (momenta * (depth - source)).astype(jnp.float32) * (1.0 / nz)
    angle = (turns - jnp.floor(turns)) * (2.0 * math.pi)
    cosine = jnp.cos(angle)
    sine = jnp.sin(angle)
    sink = jnp.where(backward, second, first)
    other = jnp.where(backward, first, second)
    column = jnp.zeros(shape, jnp.int32)
    power = jnp.zeros(shape, jnp.int32)
    for g in range(ng):
        for s in range(4):
            here = (gamma == g) & (sink == s)
            column = jnp.where(here, perm[g, s], column)
            power = jnp.where(here, phase[g, s], power)
    quarter = power - out_part + jnp.where(backward, -in_part, in_part)
    quarter = quarter & 3
    value = jnp.where((quarter & 1) == 0, cosine, sine)
    value = jnp.where(quarter >= 2, -value, value)
    value = jnp.where((column == other) & (entry < ndisp), value * scaling, 0.0)
    return value, jnp.abs(reach)


def add_pairs(sums, left, turned, right, start, size):
    def rows(ref, s):
        return ref[pl.ds(start + s, size // 4, stride=4), :].reshape(-1, 8, LANES)

    rights = [rows(right, u) for u in range(4)]
    out = []
    for side in (left, turned):
        for s in range(4):
            own = rows(side, s)
            out += [jnp.sum(own * other, axis=0) for other in rights]
    return out if sums is None else [x + y for x, y in zip(sums, out)]


def site_sums(sums):
    stacked = jnp.concatenate([jnp.sum(x, axis=0, keepdims=True) for x in sums], axis=0)
    return jnp.sum(stacked, axis=1, keepdims=True)


def keep(left, turned, at, size, real, imag):
    real, imag = real.reshape(-1, LANES), imag.reshape(-1, LANES)
    left[pl.ds(at, size), :] = real
    left[pl.ds(at + size, size), :] = imag
    if turned is not None:
        turned[pl.ds(at, size), :] = -imag
        turned[pl.ds(at + size, size), :] = real


def self_sums(field, left, turned, size):
    sums = None
    for c in range(3):
        keep(left, turned, 2 * size * c, size, field[0, c].astype(jnp.float32), field[1, c].astype(jnp.float32))
        sums = add_pairs(sums, left, turned, left, 2 * size * c, 2 * size)
    return site_sums(sums)


def link_at(ref):
    return [
        [
            [jnp.broadcast_to(ref[3 * a + b, pl.ds(part, 1), :].astype(jnp.float32), (8, LANES))
             for part in range(2)]
            for b in range(3)
        ]
        for a in range(3)
    ]


def carry_link(near, wilson, left, turned, size):
    for chunk in range(size // 16):
        field = [
            [
                near[part, a, pl.ds(chunk * 16, 16), :].astype(jnp.float32).reshape(2, 8, LANES)
                for a in range(3)
            ]
            for part in range(2)
        ]
        for b in range(3):
            real = sum(field[0][a] * wilson[a][b][0] + field[1][a] * wilson[a][b][1] for a in range(3))
            imag = sum(field[1][a] * wilson[a][b][0] - field[0][a] * wilson[a][b][1] for a in range(3))
            real, imag = real.reshape(16, LANES), imag.reshape(16, LANES)
            at = 2 * size * b + chunk * 16
            left[pl.ds(at, 16), :] = real
            left[pl.ds(at + size, 16), :] = imag
            turned[pl.ds(at, 16), :] = -imag
            turned[pl.ds(at + size, 16), :] = real


def pair_sums(far, left, turned, right, size, before):
    sums = None
    for c in range(3):
        before(c)
        keep(right, None, 2 * size * c, size, far[0, c].astype(jnp.float32), far[1, c].astype(jnp.float32))
        sums = add_pairs(sums, left, turned, right, 2 * size * c, 2 * size)
    return site_sums(sums)


def row_of(totals, table, reach):
    chosen = jnp.zeros(table.shape, jnp.float32)
    for k, total in enumerate(totals):
        chosen = jnp.where(reach == k, total, chosen)
    return jnp.sum(chosen * table, axis=0, keepdims=True)


def kernel(sizes, scaling, ranks, helped, *refs):
    refs = list(refs)
    prop, links, src_h, disp_h, mom_h, perm_h, phase_h, out = refs[:8]
    near, near_links, far, far_links, left, turned, right = refs[8:15]
    rest = refs[15:]
    heap = heap_links = heap_left = heap_turned = heap_tables = None
    if helped:
        heap, heap_links, heap_left, heap_turned, heap_tables = rest[:5]
        rest = rest[5:]
    src, disp, mom, perm, phase, gathered = rest[:6]
    local_sem, s_send, s_recv, a_recv, low_sem, line_sem, plane_sem = rest[6:13]
    rest = rest[13:]
    heap_recv = None
    if helped:
        heap_recv, rest = rest[0], rest[1:]
    link_sems = rest
    ndisp, ng, np_, nz = sizes
    nta, ngz, ngy = ranks
    nsteps = (ndisp - 1) // 2
    size = near.shape[2]
    lane_rows = gathered.shape[1]
    ta, gz, gy = lax.axis_index("ta"), lax.axis_index("gz"), lax.axis_index("gy")
    place = (ta * ngz + gz) * ngy + gy

    loads = [
        pltpu.make_async_copy(a, b, local_sem.at[min(i, 2)])
        for i, (a, b) in enumerate(
            [(prop.at[:, c], near.at[:, c]) for c in range(3)] + [(links, near_links)]
        )
    ]
    smalls = [
        pltpu.make_async_copy(a, b, local_sem.at[0])
        for a, b in [(src_h, src), (disp_h, disp), (mom_h, mom), (perm_h, perm), (phase_h, phase)]
    ]

    lines = [
        (gz, ngz, lambda i: (ta, i, gy)),
        (gy, ngy, lambda i: (ta, gz, i)),
        (ta, nta, lambda i: (i, gz, gy)),
    ]

    def greet(semaphore, at):
        pl.semaphore_signal(semaphore, inc=1, device_id=at, device_id_type=MESH)

    def greet_span(semaphore, line, low, high):
        lax.fori_loop(low, high, lambda i, carry: (greet(semaphore, line[2](i)), carry)[1], 0)

    def greet_line(semaphore, line):
        greet_span(semaphore, line, 0, line[0])
        greet_span(semaphore, line, line[0] + 1, line[1])

    count = nta * ngz * ngy
    barrier = pltpu.get_barrier_semaphore()
    for k in range(1, nsteps + 1):
        @pl.when(gz + k >= ngz)
        def _():
            greet(barrier, (ta, gz + k - ngz, gy))
    for load in loads:
        load.start()
    for line in lines:
        greet_span(barrier, line, line[0] + 1, line[1])
    nroots = min(2, ngz)
    is_root = (ta + gy == 0) & (gz < nroots)
    helper_at = (0, nroots - 1, 0)
    is_helper = (ta + gy == 0) & (gz == nroots - 1)
    is_distant = (ta == nta - 1) & (gy == ngy - 1)
    inner = lax.rem(gz, 2) == 0
    is_served = is_distant & jnp.logical_not(inner)
    served = list(range(1, ngz, 2)) if helped else []

    def place_of(z):
        return ((nta - 1) * ngz + z) * ngy + ngy - 1

    @pl.when(is_root)
    def _():
        def one(step, carry):
            at = (step // (ngz * ngy), step // ngy % ngz, step % ngy)

            @pl.when(step != place)
            def _():
                greet(barrier, at)

            return carry

        lax.fori_loop(0, count, one, 0)

    pl.semaphore_wait(
        barrier,
        jnp.maximum(gz, nsteps) + gy + ta + nroots - jnp.where(is_root, 1, 0),
    )

    def target(k):
        return (ta, lax.rem(gz + ngz - k, ngz), gy)

    sends = [
        [
            pltpu.make_async_remote_copy(
                src_ref=near.at[:, c], dst_ref=far.at[k - 1, :, c], send_sem=s_send.at[0],
                recv_sem=s_recv.at[k - 1, c // 2], device_id=target(k), device_id_type=MESH)
            for c in range(3)
        ]
        for k in range(1, nsteps + 1)
    ]
    u_send, u_recv = link_sems if link_sems else (None, None)
    link_sends = [
        pltpu.make_async_remote_copy(
            src_ref=near_links, dst_ref=far_links.at[k - 1], send_sem=u_send.at[k - 1],
            recv_sem=u_recv.at[k - 1], device_id=target(k), device_id_type=MESH)
        for k in range(1, nsteps)
    ]
    for c in range(3):
        loads[c].wait()
        if c == 2:
            loads[3].wait()
        for copies in sends:
            copies[c].start()
    if helped:
        def to_helper(source, slot, semaphore):
            pltpu.make_async_remote_copy(
                src_ref=source, dst_ref=slot, send_sem=s_send.at[0], recv_sem=semaphore,
                device_id=helper_at, device_id_type=MESH).start()

        @pl.when(is_served)
        def _():
            to_helper(near, heap.at[gz], heap_recv.at[gz // 2])

        @pl.when(is_distant & (gz == served[0] + 1))
        def _():
            for i, piece in enumerate(PIECES):
                to_helper(near.at[:, pl.ds(*piece)], heap.at[gz, :, pl.ds(*piece)], heap_recv.at[len(served) + i])

        @pl.when(is_distant & inner & (gz != served[0] + 1))
        def _():
            slot = lax.rem(gz + ngz - 1, ngz) // 2
            to_helper(near, heap.at[gz], heap_recv.at[len(PIECES) + len(served) + slot - 1])
    for line in lines:
        greet_span(low_sem.at[0], line, 0, line[0])
    if helped:
        @pl.when(is_served)
        def _():
            to_helper(near_links, heap_links.at[gz // 2], heap_recv.at[gz // 2])
    for small in smalls:
        small.start()
    for copy in link_sends:
        copy.start()
    totals = [self_sums(near, left, turned, size)]
    for small in smalls:
        small.wait()
    later = (ngz - 1 - gz) + (ngy - 1 - gy) + (nta - 1 - ta)
    outer = jnp.logical_not(inner)
    early = outer | (gy == ngy - 1)

    def meet_depth():
        @pl.when(later > 0)
        def _():
            pl.semaphore_wait(low_sem.at[0], later)

        greet_line(line_sem.at[0], lines[0])

    def meet_across():
        pl.semaphore_wait(line_sem.at[0], ngz - 1)
        greet_line(plane_sem.at[0], lines[2])

    pl.when(early)(meet_depth)
    tables = [
        weights(h, sizes, (src, disp, mom, perm, phase), (ta, gz), scaling)
        for h in range(lane_rows)
    ]

    if helped:
        @pl.when(is_helper)
        def _():
            for z in served:
                for h in range(lane_rows):
                    heap_tables[z // 2, h] = weights(
                        h, sizes, (src, disp, mom, perm, phase), (nta - 1, z), scaling)[0]

    wilson = None
    for k in range(1, nsteps + 1):
        if k == 1:
            wilson = link_at(near_links)
        else:
            link_sends[k - 2].wait_recv()
            step = link_at(far_links.at[k - 2])
            wilson = [
                [
                    [
                        sum(wilson[a][c][0] * step[c][b][0] - wilson[a][c][1] * step[c][b][1] for c in range(3)),
                        sum(wilson[a][c][0] * step[c][b][1] + wilson[a][c][1] * step[c][b][0] for c in range(3)),
                    ]
                    for b in range(3)
                ]
                for a in range(3)
            ]
        carry_link(near, wilson, left, turned, size)

        def before(c):
            for i, piece in enumerate(PIECES):
                if c == piece[0]:
                    if k == nsteps and i == len(PIECES) - 1:
                        pl.when(outer)(meet_across)
                    part = far.at[k - 1, :, pl.ds(*piece)]
                    pltpu.make_async_copy(part, part, s_recv.at[k - 1, i]).wait()

        totals.append(pair_sums(far.at[k - 1], left, turned, right, size, before))

    for h in range(lane_rows):
        gathered[place, pl.ds(h, 1), :] = row_of(totals, *tables[h])

    def give(at, row=place):
        pltpu.make_async_remote_copy(
            src_ref=gathered.at[row], dst_ref=gathered.at[row], send_sem=s_send.at[0],
            recv_sem=a_recv.at[0], device_id=at, device_id_type=MESH).start()

    for root in range(nroots):
        @pl.when((place != root * ngy) & jnp.logical_not(is_served & helped))
        def _():
            give((0, root, 0))
    pl.when(jnp.logical_not(early))(meet_depth)
    pl.when(inner)(meet_across)

    pl.semaphore_wait(plane_sem.at[0], nta - 1)
    each(ranks, place, nroots, give)
    if helped:
        @pl.when(is_helper)
        def _():
            first = []
            for z in served:
                slot = z // 2
                both = heap_left.at[slot, pl.ds(0, 3 * size + 9)]
                pltpu.make_async_copy(both, both, heap_recv.at[slot]).wait()
                first.append(self_sums(heap.at[z], heap_left.at[slot], heap_turned.at[slot], size))
                carry_link(heap.at[z], link_at(heap_links.at[slot]), heap_left.at[slot], heap_turned.at[slot], size)
            for z in reversed(served):
                slot, other = z // 2, (z + 1) % ngz

                def before(c):
                    for i, piece in enumerate(PIECES):
                        if c == 0 == i and slot > 0:
                            pltpu.make_async_copy(
                                heap.at[other], heap.at[other], heap_recv.at[len(PIECES) + len(served) + slot - 1]).wait()
                        if c == piece[0] and slot == 0:
                            part = heap.at[other, :, pl.ds(*piece)]
                            pltpu.make_async_copy(part, part, heap_recv.at[len(served) + i]).wait()

                pair = pair_sums(
                    heap.at[other], heap_left.at[slot], heap_turned.at[slot], right, size, before)
                for h in range(lane_rows):
                    gathered[place_of(z), pl.ds(h, 1), :] = row_of(
                        [first[slot], pair], heap_tables[slot, h], tables[h][1])
                for root in range(nroots - 1):
                    give((0, root, 0), place_of(z))

    def rows_done(semaphore, rows):
        if rows > 0:
            pltpu.make_async_copy(gathered.at[pl.ds(0, rows)], gathered.at[pl.ds(0, rows)], semaphore).wait()

    mine = len(served)
    if helped:
        pl.when(is_helper)(lambda: rows_done(a_recv.at[0], count - 1 - mine))
        pl.when(jnp.logical_not(is_helper))(lambda: rows_done(a_recv.at[0], count - 1))
    else:
        rows_done(a_recv.at[0], count - 1)
    for t in range(nta):
        for h in range(lane_rows):
            total = row_sum(gathered, t * ngz * ngy, ngz * ngy, h)
            low = h * (LANES // np_)
            for row in range(low, min(low + LANES // np_, out.shape[1]), 8):
                shift = (1 + row - low) * np_
                out[t, pl.ds(row, 8), :] = pltpu.roll(total, shift, 1, stride=np_, stride_axis=0)[:, :np_]
    for copy in link_sends:
        copy.wait_send()
    pltpu.make_async_copy(far, far, s_send.at[0]).wait()
    if helped:
        @pl.when(is_distant)
        def _():
            pltpu.make_async_copy(near, near, s_send.at[0]).wait()

        @pl.when(is_served)
        def _():
            pltpu.make_async_copy(near_links, near_links, s_send.at[0]).wait()

        pl.when(is_helper)(lambda: rows_done(s_send.at[0], mine * (nroots - 1)))
        pl.when(jnp.logical_not(is_served))(lambda: rows_done(s_send.at[0], nroots))
        rows_done(s_send.at[0], count - 1 - nroots)
    else:
        rows_done(s_send.at[0], count - 1)


def row_sum(ref, start, size, h):
    if size > 32:
        total = jnp.sum(ref[pl.ds(start, size), pl.ds(h, 1), :], axis=0)
        return jnp.broadcast_to(total, (8, LANES))
    terms = [jnp.broadcast_to(ref[start + i, pl.ds(h, 1), :], (8, LANES)) for i in range(size)]
    while len(terms) > 1:
        terms = [sum(terms[i:i + 2]) for i in range(0, len(terms), 2)]
    return terms[0]


def each(ranks, place, start, act):
    nta, ngz, ngy = ranks
    count = nta * ngz * ngy

    def one(step, along):
        beside = step // (nta * ngz)
        across = step // ngz % nta

        @pl.when(place != (across * ngz + along) * ngy + beside)
        def _():
            act((across, along, beside))

    if count > 64:
        lax.fori_loop(start, count, lambda step, carry: (one(step, step % ngz), carry)[1], 0)
        return
    for step in range(start, count):
        one(step, step % ngz)


def body(ranks, propagator, links, source_z, displacements, momenta, gamma_perm, gamma_phase):
    nta, ngz, ngy = ranks
    sites = propagator.shape[6]
    ndisp, np_, ng = displacements.shape[0], momenta.shape[0], gamma_perm.shape[0]
    nsteps = (ndisp - 1) // 2
    sizes = (ndisp, ng, np_, ngz)
    scaling = 1.0 / (24.0 * math.sqrt(sites * ngy * ngz))
    field = jnp.transpose(propagator, (0, 2, 3, 4, 5, 1, 6)).reshape(2, 3, -1, sites)
    link = jnp.transpose(links, (1, 2, 3, 4, 0, 5)).reshape(9, 2, sites)
    size = field.shape[2]
    regular = pltpu.SemaphoreType.REGULAR
    lane_rows = -(-ndisp * ng * np_ * 2 // LANES)
    more = max(nsteps - 1, 1)
    dma = pltpu.SemaphoreType.DMA
    helped = nsteps == 1 and ngz == 4 and nta * ngy > 1
    pairs = ngz // 2
    heaps = [
        pltpu.VMEM((ngz, 2, 3, size, sites), jnp.bfloat16),
        pltpu.VMEM((pairs, 9, 2, sites), jnp.bfloat16),
        pltpu.VMEM((pairs, 6 * size, sites), jnp.float32),
        pltpu.VMEM((pairs, 6 * size, sites), jnp.float32),
        pltpu.VMEM((pairs, lane_rows, 32, LANES), jnp.float32),
    ] if helped else []
    heap_sems = [dma((2 * pairs - 1 + len(PIECES),))] if helped else []
    reduced = pl.pallas_call(
        functools.partial(kernel, sizes, scaling, ranks, helped),
        out_shape=pltpu.VMEM((nta, ndisp * ng * 2, np_), jnp.float32),
        in_specs=[pl.BlockSpec(memory_space=pltpu.HBM)] * 7,
        out_specs=pl.BlockSpec(memory_space=pltpu.VMEM),
        scratch_shapes=[
            pltpu.VMEM((2, 3, size, sites), jnp.bfloat16),
            pltpu.VMEM((9, 2, sites), jnp.bfloat16),
            pltpu.VMEM((nsteps, 2, 3, size, sites), jnp.bfloat16),
            pltpu.VMEM((more, 9, 2, sites), jnp.bfloat16),
            pltpu.VMEM((6 * size, sites), jnp.float32),
            pltpu.VMEM((6 * size, sites), jnp.float32),
            pltpu.VMEM((6 * size, sites), jnp.float32),
            *heaps,
            pltpu.SMEM(source_z.shape, jnp.int32),
            pltpu.SMEM(displacements.shape, jnp.int32),
            pltpu.SMEM(momenta.shape, jnp.int32),
            pltpu.SMEM(gamma_perm.shape, jnp.int32),
            pltpu.SMEM(gamma_phase.shape, jnp.int32),
            pltpu.VMEM((nta * ngz * ngy, lane_rows, LANES), jnp.float32),
            dma((3,)), dma((1,)), dma((nsteps, len(PIECES))),
            dma((1,)), regular((1,)), regular((1,)), regular((1,)),
            *heap_sems,
        ] + [dma((nsteps - 1,))] * (2 if nsteps > 1 else 0),
        compiler_params=pltpu.CompilerParams(collective_id=0, has_side_effects=True),
    )(field, link, source_z, displacements, momenta, gamma_perm, gamma_phase)
    return jnp.swapaxes(reduced.reshape(nta, ndisp, ng, 2, np_), 3, 4)


def solution(mesh):
    placed = (
        P(None, None, None, None, "ta", "gz", "gy"),
        P(None, None, None, "ta", "gz", "gy"),
        P(),
        P(),
        P(),
        P(),
        P(),
    )
    ranks = tuple(mesh.shape[axis] for axis in ("ta", "gz", "gy"))
    return jax.shard_map(
        functools.partial(body, ranks), mesh=mesh, in_specs=placed, out_specs=P(), check_vma=False
    )
```

```python
import functools
import math

import jax
import jax.numpy as jnp
from jax import lax
from jax.experimental import pallas as pl
from jax.experimental.pallas import tpu as pltpu
from jax.sharding import PartitionSpec as P

MESH = pl.DeviceIdType.MESH
PIECES = ((0, 2), (2, 1))
LANES = 128


def weights(lane_row, sizes, smem, place, scaling):
    ndisp, ng, np_, nz = sizes
    src, disp, mom, perm, phase = smem
    slice_at, depth_at = place
    nsteps = (ndisp - 1) // 2
    shape = (32, LANES)
    lane = lax.broadcasted_iota(jnp.int32, shape, 1)
    momentum = lane & (np_ - 1)
    lane = lane_row * LANES + LANES - np_ - (lane - momentum)
    row = lax.broadcasted_iota(jnp.int32, shape, 0)
    out_part = (lane // np_) & 1
    gamma = (lane // (2 * np_)) & (ng - 1)
    entry = lane // (2 * np_ * ng)
    in_part = row // 16
    first = (row // 4) & 3
    second = row & 3
    reach = jnp.full(shape, 2 * nsteps + 1, jnp.int32)
    for j in range(ndisp):
        reach = jnp.where(entry == j, disp[j] - nsteps, reach)
    backward = reach < 0
    momenta = jnp.zeros(shape, jnp.int32)
    source = jnp.zeros(shape, jnp.int32)
    for p in range(np_):
        momenta = jnp.where(momentum == p, mom[p], momenta)
        source = jnp.where(momentum == p, src[slice_at, p], source)
    depth = depth_at - jnp.where(backward, reach, 0)
    turns = (momenta * (depth - source)).astype(jnp.float32) * (1.0 / nz)
    angle = (turns - jnp.floor(turns)) * (2.0 * math.pi)
    cosine = jnp.cos(angle)
    sine = jnp.sin(angle)
    sink = jnp.where(backward, second, first)
    other = jnp.where(backward, first, second)
    column = jnp.zeros(shape, jnp.int32)
    power = jnp.zeros(shape, jnp.int32)
    for g in range(ng):
        for s in range(4):
            here = (gamma == g) & (sink == s)
            column = jnp.where(here, perm[g, s], column)
            power = jnp.where(here, phase[g, s], power)
    quarter = power - out_part + jnp.where(backward, -in_part, in_part)
    quarter = quarter & 3
    value = jnp.where((quarter & 1) == 0, cosine, sine)
    value = jnp.where(quarter >= 2, -value, value)
    value = jnp.where((column == other) & (entry < ndisp), value * scaling, 0.0)
    return value, jnp.abs(reach)


def add_pairs(sums, left, turned, right, start, size):
    def rows(ref, s):
        return ref[pl.ds(start + s, size // 4, stride=4), :].reshape(-1, 8, LANES)

    rights = [rows(right, u) for u in range(4)]
    out = []
    for side in (left, turned):
        for s in range(4):
            own = rows(side, s)
            out += [jnp.sum(own * other, axis=0) for other in rights]
    return out if sums is None else [x + y for x, y in zip(sums, out)]


def site_sums(sums):
    row = lax.broadcasted_iota(jnp.int32, (8, LANES), 0)
    for step in (1, 2, 4):
        first = (row & step) == 0
        pairs = zip(sums[::2], sums[1::2])
        sums = [
            jnp.where(first, x, y) + pltpu.roll(jnp.where(first, y, x), step, 0)
            for x, y in pairs
        ]
    return jnp.sum(jnp.concatenate(sums, axis=0), axis=1, keepdims=True)


def keep(left, turned, at, size, real, imag):
    real, imag = real.reshape(-1, LANES), imag.reshape(-1, LANES)
    left[pl.ds(at, size), :] = real
    left[pl.ds(at + size, size), :] = imag
    if turned is not None:
        turned[pl.ds(at, size), :] = -imag
        turned[pl.ds(at + size, size), :] = real


def self_sums(field, left, turned, size):
    sums = None
    for c in range(3):
        keep(left, turned, 2 * size * c, size, field[0, c].astype(jnp.float32), field[1, c].astype(jnp.float32))
        sums = add_pairs(sums, left, turned, left, 2 * size * c, 2 * size)
    return site_sums(sums)


def link_at(ref):
    return [
        [
            [jnp.broadcast_to(ref[3 * a + b, pl.ds(part, 1), :].astype(jnp.float32), (8, LANES))
             for part in range(2)]
            for b in range(3)
        ]
        for a in range(3)
    ]


def carry_link(near, wilson, left, turned, size):
    for chunk in range(size // 16):
        field = [
            [
                near[part, a, pl.ds(chunk * 16, 16), :].astype(jnp.float32).reshape(2, 8, LANES)
                for a in range(3)
            ]
            for part in range(2)
        ]
        for b in range(3):
            real = sum(field[0][a] * wilson[a][b][0] + field[1][a] * wilson[a][b][1] for a in range(3))
            imag = sum(field[1][a] * wilson[a][b][0] - field[0][a] * wilson[a][b][1] for a in range(3))
            real, imag = real.reshape(16, LANES), imag.reshape(16, LANES)
            at = 2 * size * b + chunk * 16
            left[pl.ds(at, 16), :] = real
            left[pl.ds(at + size, 16), :] = imag
            turned[pl.ds(at, 16), :] = -imag
            turned[pl.ds(at + size, 16), :] = real


def pair_sums(far, left, turned, right, size, before):
    sums = None
    for c in range(3):
        before(c)
        keep(right, None, 2 * size * c, size, far[0, c].astype(jnp.float32), far[1, c].astype(jnp.float32))
        sums = add_pairs(sums, left, turned, right, 2 * size * c, 2 * size)
    return site_sums(sums)


def row_of(totals, table, reach):
    chosen = jnp.zeros(table.shape, jnp.float32)
    for k, total in enumerate(totals):
        chosen = jnp.where(reach == k, total, chosen)
    return jnp.sum(chosen * table, axis=0, keepdims=True)


def kernel(sizes, scaling, ranks, helped, *refs):
    refs = list(refs)
    prop, links, src_h, disp_h, mom_h, perm_h, phase_h, out = refs[:8]
    near, near_links, far, far_links, left, turned, right = refs[8:15]
    rest = refs[15:]
    heap = heap_links = heap_left = heap_turned = heap_tables = None
    if helped:
        heap, heap_links, heap_left, heap_turned, heap_tables = rest[:5]
        rest = rest[5:]
    src, disp, mom, perm, phase, gathered = rest[:6]
    local_sem, s_send, s_recv, a_recv, low_sem, line_sem, plane_sem = rest[6:13]
    rest = rest[13:]
    heap_recv = None
    if helped:
        heap_recv, rest = rest[0], rest[1:]
    link_sems = rest
    ndisp, ng, np_, nz = sizes
    nta, ngz, ngy = ranks
    nsteps = (ndisp - 1) // 2
    size = near.shape[2]
    lane_rows = gathered.shape[1]
    ta, gz, gy = lax.axis_index("ta"), lax.axis_index("gz"), lax.axis_index("gy")
    place = (ta * ngz + gz) * ngy + gy

    loads = [
        pltpu.make_async_copy(a, b, local_sem.at[min(i, 2)])
        for i, (a, b) in enumerate(
            [(prop.at[:, c], near.at[:, c]) for c in range(3)] + [(links, near_links)]
        )
    ]
    smalls = [
        pltpu.make_async_copy(a, b, local_sem.at[0])
        for a, b in [(src_h, src), (disp_h, disp), (mom_h, mom), (perm_h, perm), (phase_h, phase)]
    ]

    lines = [
        (gz, ngz, lambda i: (ta, i, gy)),
        (gy, ngy, lambda i: (ta, gz, i)),
        (ta, nta, lambda i: (i, gz, gy)),
    ]

    def greet(semaphore, at):
        pl.semaphore_signal(semaphore, inc=1, device_id=at, device_id_type=MESH)

    def greet_span(semaphore, line, low, high):
        lax.fori_loop(low, high, lambda i, carry: (greet(semaphore, line[2](i)), carry)[1], 0)

    def greet_line(semaphore, line):
        greet_span(semaphore, line, 0, line[0])
        greet_span(semaphore, line, line[0] + 1, line[1])

    count = nta * ngz * ngy
    barrier = pltpu.get_barrier_semaphore()
    for k in range(1, nsteps + 1):
        @pl.when(gz + k >= ngz)
        def _():
            greet(barrier, (ta, gz + k - ngz, gy))
    for load in loads:
        load.start()
    for line in lines:
        greet_span(barrier, line, line[0] + 1, line[1])
    nroots = min(2, ngz)
    is_root = (ta + gy == 0) & (gz < nroots)
    helper_at = (0, nroots - 1, 0)
    is_helper = (ta + gy == 0) & (gz == nroots - 1)
    is_distant = (ta == nta - 1) & (gy == ngy - 1)
    inner = lax.rem(gz, 2) == 0
    is_served = is_distant & jnp.logical_not(inner)
    served = list(range(1, ngz, 2)) if helped else []

    def place_of(z):
        return ((nta - 1) * ngz + z) * ngy + ngy - 1

    @pl.when(is_root)
    def _():
        def one(step, carry):
            at = (step // (ngz * ngy), step // ngy % ngz, step % ngy)

            @pl.when(step != place)
            def _():
                greet(barrier, at)

            return carry

        lax.fori_loop(0, count, one, 0)

    pl.semaphore_wait(
        barrier,
        jnp.maximum(gz, nsteps) + gy + ta + nroots - jnp.where(is_root, 1, 0),
    )

    def target(k):
        return (ta, lax.rem(gz + ngz - k, ngz), gy)

    sends = [
        [
            pltpu.make_async_remote_copy(
                src_ref=near.at[:, c], dst_ref=far.at[k - 1, :, c], send_sem=s_send.at[0],
                recv_sem=s_recv.at[k - 1, c // 2], device_id=target(k), device_id_type=MESH)
            for c in range(3)
        ]
        for k in range(1, nsteps + 1)
    ]
    u_send, u_recv = link_sems if link_sems else (None, None)
    link_sends = [
        pltpu.make_async_remote_copy(
            src_ref=near_links, dst_ref=far_links.at[k - 1], send_sem=u_send.at[k - 1],
            recv_sem=u_recv.at[k - 1], device_id=target(k), device_id_type=MESH)
        for k in range(1, nsteps)
    ]
    def to_helper(source, slot, semaphore):
        pltpu.make_async_remote_copy(
            src_ref=source, dst_ref=slot, send_sem=s_send.at[0], recv_sem=heap_recv.at[semaphore],
            device_id=helper_at, device_id_type=MESH).start()

    def field_semaphore(c):
        slot = lax.rem(gz + ngz - 1, ngz) // 2
        beyond = jnp.where(slot == 0, c // 2, len(PIECES) + slot - 1)
        return jnp.where(inner, len(served) + beyond, gz // 2)

    for c in range(3):
        loads[c].wait()
        if c == 2:
            loads[3].wait()
        for copies in sends:
            copies[c].start()
        if helped:
            pl.when(is_distant)(
                lambda: to_helper(near.at[:, c], heap.at[gz, :, c], field_semaphore(c)))
    for line in lines:
        greet_span(low_sem.at[0], line, 0, line[0])
    if helped:
        @pl.when(is_served)
        def _():
            to_helper(near_links, heap_links.at[gz // 2], gz // 2)
    for small in smalls:
        small.start()
    for copy in link_sends:
        copy.start()
    totals = [self_sums(near, left, turned, size)]
    for small in smalls:
        small.wait()
    later = (ngz - 1 - gz) + (ngy - 1 - gy) + (nta - 1 - ta)
    outer = jnp.logical_not(inner)
    early = outer | (gy == ngy - 1)

    def meet_depth():
        @pl.when(later > 0)
        def _():
            pl.semaphore_wait(low_sem.at[0], later)

        greet_line(line_sem.at[0], lines[0])

    def meet_across():
        pl.semaphore_wait(line_sem.at[0], ngz - 1)
        greet_line(plane_sem.at[0], lines[2])

    pl.when(early)(meet_depth)
    tables = [
        weights(h, sizes, (src, disp, mom, perm, phase), (ta, gz), scaling)
        for h in range(lane_rows)
    ]

    if helped:
        @pl.when(is_helper)
        def _():
            for z in served:
                for h in range(lane_rows):
                    heap_tables[z // 2, h] = weights(
                        h, sizes, (src, disp, mom, perm, phase), (nta - 1, z), scaling)[0]

    wilson = None
    for k in range(1, nsteps + 1):
        if k == 1:
            wilson = link_at(near_links)
        else:
            link_sends[k - 2].wait_recv()
            step = link_at(far_links.at[k - 2])
            wilson = [
                [
                    [
                        sum(wilson[a][c][0] * step[c][b][0] - wilson[a][c][1] * step[c][b][1] for c in range(3)),
                        sum(wilson[a][c][0] * step[c][b][1] + wilson[a][c][1] * step[c][b][0] for c in range(3)),
                    ]
                    for b in range(3)
                ]
                for a in range(3)
            ]
        carry_link(near, wilson, left, turned, size)

        def before(c):
            for i, piece in enumerate(PIECES):
                if c == piece[0]:
                    if k == nsteps and i == len(PIECES) - 1:
                        pl.when(outer)(meet_across)
                    part = far.at[k - 1, :, pl.ds(*piece)]
                    pltpu.make_async_copy(part, part, s_recv.at[k - 1, i]).wait()

        totals.append(pair_sums(far.at[k - 1], left, turned, right, size, before))

    for h in range(lane_rows):
        gathered[place, pl.ds(h, 1), :] = row_of(totals, *tables[h])

    def give(at, row=place):
        pltpu.make_async_remote_copy(
            src_ref=gathered.at[row], dst_ref=gathered.at[row], send_sem=s_send.at[0],
            recv_sem=a_recv.at[0], device_id=at, device_id_type=MESH).start()

    for root in range(nroots):
        @pl.when((place != root * ngy) & jnp.logical_not(is_served & helped))
        def _():
            give((0, root, 0))
    pl.when(jnp.logical_not(early))(meet_depth)
    pl.when(inner)(meet_across)

    pl.semaphore_wait(plane_sem.at[0], nta - 1)
    each(ranks, place, nroots, give)
    if helped:
        @pl.when(is_helper)
        def _():
            first = []
            for z in served:
                slot = z // 2
                both = heap_left.at[slot, pl.ds(0, 3 * size + 9)]
                pltpu.make_async_copy(both, both, heap_recv.at[slot]).wait()
                first.append(self_sums(heap.at[z], heap_left.at[slot], heap_turned.at[slot], size))
                carry_link(heap.at[z], link_at(heap_links.at[slot]), heap_left.at[slot], heap_turned.at[slot], size)
            for z in reversed(served):
                slot, other = z // 2, (z + 1) % ngz

                def before(c):
                    for i, piece in enumerate(PIECES):
                        if c == 0 == i and slot > 0:
                            pltpu.make_async_copy(
                                heap.at[other], heap.at[other], heap_recv.at[len(PIECES) + len(served) + slot - 1]).wait()
                        if c == piece[0] and slot == 0:
                            part = heap.at[other, :, pl.ds(*piece)]
                            pltpu.make_async_copy(part, part, heap_recv.at[len(served) + i]).wait()

                pair = pair_sums(
                    heap.at[other], heap_left.at[slot], heap_turned.at[slot], right, size, before)
                for h in range(lane_rows):
                    gathered[place_of(z), pl.ds(h, 1), :] = row_of(
                        [first[slot], pair], heap_tables[slot, h], tables[h][1])
                for root in range(nroots - 1):
                    give((0, root, 0), place_of(z))

    def rows_done(semaphore, rows):
        if rows > 0:
            pltpu.make_async_copy(gathered.at[pl.ds(0, rows)], gathered.at[pl.ds(0, rows)], semaphore).wait()

    mine = len(served)
    if helped:
        pl.when(is_helper)(lambda: rows_done(a_recv.at[0], count - 1 - mine))
        pl.when(jnp.logical_not(is_helper))(lambda: rows_done(a_recv.at[0], count - 1))
    else:
        rows_done(a_recv.at[0], count - 1)
    for t in range(nta):
        for h in range(lane_rows):
            total = row_sum(gathered, t * ngz * ngy, ngz * ngy, h)
            low = h * (LANES // np_)
            for row in range(low, min(low + LANES // np_, out.shape[1]), 8):
                shift = (1 + row - low) * np_
                out[t, pl.ds(row, 8), :] = pltpu.roll(total, shift, 1, stride=np_, stride_axis=0)[:, :np_]
    for copy in link_sends:
        copy.wait_send()
    pltpu.make_async_copy(far, far, s_send.at[0]).wait()
    if helped:
        @pl.when(is_distant)
        def _():
            pltpu.make_async_copy(near, near, s_send.at[0]).wait()

        @pl.when(is_served)
        def _():
            pltpu.make_async_copy(near_links, near_links, s_send.at[0]).wait()

        pl.when(is_helper)(lambda: rows_done(s_send.at[0], mine * (nroots - 1)))
        pl.when(jnp.logical_not(is_served))(lambda: rows_done(s_send.at[0], nroots))
        rows_done(s_send.at[0], count - 1 - nroots)
    else:
        rows_done(s_send.at[0], count - 1)


def row_sum(ref, start, size, h):
    if size > 32:
        total = jnp.sum(ref[pl.ds(start, size), pl.ds(h, 1), :], axis=0)
        return jnp.broadcast_to(total, (8, LANES))
    terms = [jnp.broadcast_to(ref[start + i, pl.ds(h, 1), :], (8, LANES)) for i in range(size)]
    while len(terms) > 1:
        terms = [sum(terms[i:i + 2]) for i in range(0, len(terms), 2)]
    return terms[0]


def each(ranks, place, start, act):
    nta, ngz, ngy = ranks
    count = nta * ngz * ngy

    def one(step, along):
        beside = step // (nta * ngz)
        across = step // ngz % nta

        @pl.when(place != (across * ngz + along) * ngy + beside)
        def _():
            act((across, along, beside))

    if count > 64:
        lax.fori_loop(start, count, lambda step, carry: (one(step, step % ngz), carry)[1], 0)
        return
    for step in range(start, count):
        one(step, step % ngz)


def body(ranks, propagator, links, source_z, displacements, momenta, gamma_perm, gamma_phase):
    nta, ngz, ngy = ranks
    sites = propagator.shape[6]
    ndisp, np_, ng = displacements.shape[0], momenta.shape[0], gamma_perm.shape[0]
    nsteps = (ndisp - 1) // 2
    sizes = (ndisp, ng, np_, ngz)
    scaling = 1.0 / (24.0 * math.sqrt(sites * ngy * ngz))
    field = jnp.transpose(propagator, (0, 2, 3, 4, 5, 1, 6)).reshape(2, 3, -1, sites)
    link = jnp.transpose(links, (1, 2, 3, 4, 0, 5)).reshape(9, 2, sites)
    size = field.shape[2]
    regular = pltpu.SemaphoreType.REGULAR
    lane_rows = -(-ndisp * ng * np_ * 2 // LANES)
    more = max(nsteps - 1, 1)
    dma = pltpu.SemaphoreType.DMA
    helped = nsteps == 1 and ngz == 4 and nta * ngy > 1
    pairs = ngz // 2
    heaps = [
        pltpu.VMEM((ngz, 2, 3, size, sites), jnp.bfloat16),
        pltpu.VMEM((pairs, 9, 2, sites), jnp.bfloat16),
        pltpu.VMEM((pairs, 6 * size, sites), jnp.float32),
        pltpu.VMEM((pairs, 6 * size, sites), jnp.float32),
        pltpu.VMEM((pairs, lane_rows, 32, LANES), jnp.float32),
    ] if helped else []
    heap_sems = [dma((2 * pairs - 1 + len(PIECES),))] if helped else []
    reduced = pl.pallas_call(
        functools.partial(kernel, sizes, scaling, ranks, helped),
        out_shape=pltpu.VMEM((nta, ndisp * ng * 2, np_), jnp.float32),
        in_specs=[pl.BlockSpec(memory_space=pltpu.HBM)] * 7,
        out_specs=pl.BlockSpec(memory_space=pltpu.VMEM),
        scratch_shapes=[
            pltpu.VMEM((2, 3, size, sites), jnp.bfloat16),
            pltpu.VMEM((9, 2, sites), jnp.bfloat16),
            pltpu.VMEM((nsteps, 2, 3, size, sites), jnp.bfloat16),
            pltpu.VMEM((more, 9, 2, sites), jnp.bfloat16),
            pltpu.VMEM((6 * size, sites), jnp.float32),
            pltpu.VMEM((6 * size, sites), jnp.float32),
            pltpu.VMEM((6 * size, sites), jnp.float32),
            *heaps,
            pltpu.SMEM(source_z.shape, jnp.int32),
            pltpu.SMEM(displacements.shape, jnp.int32),
            pltpu.SMEM(momenta.shape, jnp.int32),
            pltpu.SMEM(gamma_perm.shape, jnp.int32),
            pltpu.SMEM(gamma_phase.shape, jnp.int32),
            pltpu.VMEM((nta * ngz * ngy, lane_rows, LANES), jnp.float32),
            dma((3,)), dma((1,)), dma((nsteps, len(PIECES))),
            dma((1,)), regular((1,)), regular((1,)), regular((1,)),
            *heap_sems,
        ] + [dma((nsteps - 1,))] * (2 if nsteps > 1 else 0),
        compiler_params=pltpu.CompilerParams(collective_id=0, has_side_effects=True),
    )(field, link, source_z, displacements, momenta, gamma_perm, gamma_phase)
    return jnp.swapaxes(reduced.reshape(nta, ndisp, ng, 2, np_), 3, 4)


def solution(mesh):
    placed = (
        P(None, None, None, None, "ta", "gz", "gy"),
        P(None, None, None, "ta", "gz", "gy"),
        P(),
        P(),
        P(),
        P(),
        P(),
    )
    ranks = tuple(mesh.shape[axis] for axis in ("ta", "gz", "gy"))
    return jax.shard_map(
        functools.partial(body, ranks), mesh=mesh, in_specs=placed, out_specs=P(), check_vma=False
    )
```

```python
import functools
import math

import jax
import jax.numpy as jnp
from jax import lax
from jax.experimental import pallas as pl
from jax.experimental.pallas import tpu as pltpu
from jax.sharding import PartitionSpec as P

MESH = pl.DeviceIdType.MESH
PIECES = ((0, 2), (2, 1))
LANES = 128


def weights(lane_row, sizes, smem, place, scaling):
    ndisp, ng, np_, nz = sizes
    src, disp, mom, perm, phase = smem
    slice_at, depth_at = place
    nsteps = (ndisp - 1) // 2
    shape = (32, LANES)
    lane = lax.broadcasted_iota(jnp.int32, shape, 1)
    momentum = lane & (np_ - 1)
    lane = lane_row * LANES + LANES - np_ - (lane - momentum)
    row = lax.broadcasted_iota(jnp.int32, shape, 0)
    out_part = (lane // np_) & 1
    gamma = (lane // (2 * np_)) & (ng - 1)
    entry = lane // (2 * np_ * ng)
    in_part = row // 16
    first = (row // 4) & 3
    second = row & 3
    reach = jnp.full(shape, 2 * nsteps + 1, jnp.int32)
    for j in range(ndisp):
        reach = jnp.where(entry == j, disp[j] - nsteps, reach)
    backward = reach < 0
    momenta = jnp.zeros(shape, jnp.int32)
    source = jnp.zeros(shape, jnp.int32)
    for p in range(np_):
        momenta = jnp.where(momentum == p, mom[p], momenta)
        source = jnp.where(momentum == p, src[slice_at, p], source)
    depth = depth_at - jnp.where(backward, reach, 0)
    turns = (momenta * (depth - source)).astype(jnp.float32) * (1.0 / nz)
    angle = (turns - jnp.floor(turns)) * (2.0 * math.pi)
    cosine = jnp.cos(angle)
    sine = jnp.sin(angle)
    sink = jnp.where(backward, second, first)
    other = jnp.where(backward, first, second)
    column = jnp.zeros(shape, jnp.int32)
    power = jnp.zeros(shape, jnp.int32)
    for g in range(ng):
        for s in range(4):
            here = (gamma == g) & (sink == s)
            column = jnp.where(here, perm[g, s], column)
            power = jnp.where(here, phase[g, s], power)
    quarter = power - out_part + jnp.where(backward, -in_part, in_part)
    quarter = quarter & 3
    value = jnp.where((quarter & 1) == 0, cosine, sine)
    value = jnp.where(quarter >= 2, -value, value)
    value = jnp.where((column == other) & (entry < ndisp), value * scaling, 0.0)
    return value, jnp.abs(reach)


def add_pairs(sums, left, turned, right, start, size):
    def rows(ref, s):
        return ref[pl.ds(start + s, size // 4, stride=4), :].reshape(-1, 8, LANES)

    rights = [rows(right, u) for u in range(4)]
    out = []
    for side in (left, turned):
        for s in range(4):
            own = rows(side, s)
            out += [jnp.sum(own * other, axis=0) for other in rights]
    return out if sums is None else [x + y for x, y in zip(sums, out)]


def site_sums(sums):
    row = lax.broadcasted_iota(jnp.int32, (8, LANES), 0)
    for step in (1, 2, 4):
        first = (row & step) == 0
        pairs = zip(sums[::2], sums[1::2])
        sums = [
            jnp.where(first, x, y) + pltpu.roll(jnp.where(first, y, x), step, 0)
            for x, y in pairs
        ]
    return jnp.sum(jnp.concatenate(sums, axis=0), axis=1, keepdims=True)


def keep(left, turned, at, size, real, imag):
    real, imag = real.reshape(-1, LANES), imag.reshape(-1, LANES)
    left[pl.ds(at, size), :] = real
    left[pl.ds(at + size, size), :] = imag
    if turned is not None:
        turned[pl.ds(at, size), :] = -imag
        turned[pl.ds(at + size, size), :] = real


def self_sums(field, left, turned, size):
    sums = None
    for c in range(3):
        keep(left, turned, 2 * size * c, size, field[0, c].astype(jnp.float32), field[1, c].astype(jnp.float32))
        sums = add_pairs(sums, left, turned, left, 2 * size * c, 2 * size)
    return site_sums(sums)


def link_at(ref):
    return [
        [
            [jnp.broadcast_to(ref[3 * a + b, pl.ds(part, 1), :].astype(jnp.float32), (8, LANES))
             for part in range(2)]
            for b in range(3)
        ]
        for a in range(3)
    ]


def carry_link(near, wilson, left, turned, size):
    for chunk in range(size // 16):
        field = [
            [
                near[part, a, pl.ds(chunk * 16, 16), :].astype(jnp.float32).reshape(2, 8, LANES)
                for a in range(3)
            ]
            for part in range(2)
        ]
        for b in range(3):
            real = sum(field[0][a] * wilson[a][b][0] + field[1][a] * wilson[a][b][1] for a in range(3))
            imag = sum(field[1][a] * wilson[a][b][0] - field[0][a] * wilson[a][b][1] for a in range(3))
            real, imag = real.reshape(16, LANES), imag.reshape(16, LANES)
            at = 2 * size * b + chunk * 16
            left[pl.ds(at, 16), :] = real
            left[pl.ds(at + size, 16), :] = imag
            turned[pl.ds(at, 16), :] = -imag
            turned[pl.ds(at + size, 16), :] = real


def pair_sums(far, left, turned, right, size, before):
    sums = None
    for c in range(3):
        before(c)
        keep(right, None, 2 * size * c, size, far[0, c].astype(jnp.float32), far[1, c].astype(jnp.float32))
        sums = add_pairs(sums, left, turned, right, 2 * size * c, 2 * size)
    return site_sums(sums)


def row_of(totals, table, reach):
    chosen = jnp.zeros(table.shape, jnp.float32)
    for k, total in enumerate(totals):
        chosen = jnp.where(reach == k, total, chosen)
    return jnp.sum(chosen * table, axis=0, keepdims=True)


def kernel(sizes, scaling, ranks, helped, *refs):
    refs = list(refs)
    prop, links, src_h, disp_h, mom_h, perm_h, phase_h, out = refs[:8]
    near, near_links, far, far_links, left, turned, right = refs[8:15]
    rest = refs[15:]
    heap = heap_links = heap_left = heap_turned = heap_tables = None
    if helped:
        heap, heap_links, heap_left, heap_turned, heap_tables = rest[:5]
        rest = rest[5:]
    src, disp, mom, perm, phase, gathered = rest[:6]
    local_sem, s_send, s_recv, a_recv, low_sem, line_sem, plane_sem = rest[6:13]
    rest = rest[13:]
    heap_recv = None
    if helped:
        heap_recv, rest = rest[0], rest[1:]
    link_sems = rest
    ndisp, ng, np_, nz = sizes
    nta, ngz, ngy = ranks
    nsteps = (ndisp - 1) // 2
    size = near.shape[2]
    lane_rows = gathered.shape[1]
    ta, gz, gy = lax.axis_index("ta"), lax.axis_index("gz"), lax.axis_index("gy")
    place = (ta * ngz + gz) * ngy + gy

    loads = [
        pltpu.make_async_copy(a, b, local_sem.at[min(i, 2)])
        for i, (a, b) in enumerate(
            [(prop.at[:, c], near.at[:, c]) for c in range(3)] + [(links, near_links)]
        )
    ]
    smalls = [
        pltpu.make_async_copy(a, b, local_sem.at[0])
        for a, b in [(src_h, src), (disp_h, disp), (mom_h, mom), (perm_h, perm), (phase_h, phase)]
    ]

    lines = [
        (gz, ngz, lambda i: (ta, i, gy)),
        (gy, ngy, lambda i: (ta, gz, i)),
        (ta, nta, lambda i: (i, gz, gy)),
    ]

    def greet(semaphore, at):
        pl.semaphore_signal(semaphore, inc=1, device_id=at, device_id_type=MESH)

    def greet_span(semaphore, line, low, high):
        lax.fori_loop(low, high, lambda i, carry: (greet(semaphore, line[2](i)), carry)[1], 0)

    def greet_line(semaphore, line):
        greet_span(semaphore, line, 0, line[0])
        greet_span(semaphore, line, line[0] + 1, line[1])

    count = nta * ngz * ngy
    barrier = pltpu.get_barrier_semaphore()
    for k in range(1, nsteps + 1):
        @pl.when(gz + k >= ngz)
        def _():
            greet(barrier, (ta, gz + k - ngz, gy))
    for load in loads:
        load.start()
    for line in lines:
        greet_span(barrier, line, line[0] + 1, line[1])
    nroots = min(2, ngz)
    is_root = (ta + gy == 0) & (gz < nroots)
    helper_at = (0, nroots - 1, 0)
    is_helper = (ta + gy == 0) & (gz == nroots - 1)
    is_distant = (ta == nta - 1) & (gy == ngy - 1)
    inner = lax.rem(gz, 2) == 0
    is_served = is_distant & jnp.logical_not(inner)
    served = list(range(1, ngz, 2)) if helped else []

    def place_of(z):
        return ((nta - 1) * ngz + z) * ngy + ngy - 1

    @pl.when(is_root)
    def _():
        def one(step, carry):
            at = (step // (ngz * ngy), step // ngy % ngz, step % ngy)

            @pl.when(step != place)
            def _():
                greet(barrier, at)

            return carry

        lax.fori_loop(0, count, one, 0)

    pl.semaphore_wait(
        barrier,
        jnp.maximum(gz, nsteps) + gy + ta + nroots - jnp.where(is_root, 1, 0),
    )

    def target(k):
        return (ta, lax.rem(gz + ngz - k, ngz), gy)

    sends = [
        [
            pltpu.make_async_remote_copy(
                src_ref=near.at[:, c], dst_ref=far.at[k - 1, :, c], send_sem=s_send.at[0],
                recv_sem=s_recv.at[k - 1, c // 2], device_id=target(k), device_id_type=MESH)
            for c in range(3)
        ]
        for k in range(1, nsteps + 1)
    ]
    u_send, u_recv = link_sems if link_sems else (None, None)
    link_sends = [
        pltpu.make_async_remote_copy(
            src_ref=near_links, dst_ref=far_links.at[k - 1], send_sem=u_send.at[k - 1],
            recv_sem=u_recv.at[k - 1], device_id=target(k), device_id_type=MESH)
        for k in range(1, nsteps)
    ]

    def to_helper(source, slot, semaphore):
        pltpu.make_async_remote_copy(
            src_ref=source, dst_ref=slot, send_sem=s_send.at[0], recv_sem=heap_recv.at[semaphore],
            device_id=helper_at, device_id_type=MESH).start()

    def field_semaphore(c):
        slot = jnp.where(inner, lax.rem(gz + ngz - 1, ngz), gz) // 2
        return jnp.where(inner & (slot == 0), len(served) + c // 2, slot)

    for c in range(3):
        loads[c].wait()
        if c == 2:
            loads[3].wait()
        for copies in sends:
            copies[c].start()
        if helped:
            pl.when(is_distant)(
                lambda: to_helper(near.at[:, c], heap.at[gz, :, c], field_semaphore(c)))
    for line in lines:
        greet_span(low_sem.at[0], line, 0, line[0])
    if helped:
        @pl.when(is_served)
        def _():
            to_helper(near_links, heap_links.at[gz // 2], gz // 2)
    for small in smalls:
        small.start()
    for copy in link_sends:
        copy.start()
    totals = [self_sums(near, left, turned, size)]
    for small in smalls:
        small.wait()
    later = (ngz - 1 - gz) + (ngy - 1 - gy) + (nta - 1 - ta)
    outer = jnp.logical_not(inner)
    early = outer | (gy == ngy - 1)

    def meet_depth():
        @pl.when(later > 0)
        def _():
            pl.semaphore_wait(low_sem.at[0], later)

        greet_line(line_sem.at[0], lines[0])

    def meet_across():
        pl.semaphore_wait(line_sem.at[0], ngz - 1)
        greet_line(plane_sem.at[0], lines[2])

    pl.when(early)(meet_depth)
    tables = [
        weights(h, sizes, (src, disp, mom, perm, phase), (ta, gz), scaling)
        for h in range(lane_rows)
    ]

    if helped:
        @pl.when(is_helper)
        def _():
            for z in served:
                for h in range(lane_rows):
                    heap_tables[z // 2, h] = weights(
                        h, sizes, (src, disp, mom, perm, phase), (nta - 1, z), scaling)[0]

    wilson = None
    for k in range(1, nsteps + 1):
        if k == 1:
            wilson = link_at(near_links)
        else:
            link_sends[k - 2].wait_recv()
            step = link_at(far_links.at[k - 2])
            wilson = [
                [
                    [
                        sum(wilson[a][c][0] * step[c][b][0] - wilson[a][c][1] * step[c][b][1] for c in range(3)),
                        sum(wilson[a][c][0] * step[c][b][1] + wilson[a][c][1] * step[c][b][0] for c in range(3)),
                    ]
                    for b in range(3)
                ]
                for a in range(3)
            ]
        carry_link(near, wilson, left, turned, size)

        def before(c):
            for i, piece in enumerate(PIECES):
                if c == piece[0]:
                    if k == nsteps and i == len(PIECES) - 1:
                        pl.when(outer)(meet_across)
                    part = far.at[k - 1, :, pl.ds(*piece)]
                    pltpu.make_async_copy(part, part, s_recv.at[k - 1, i]).wait()

        totals.append(pair_sums(far.at[k - 1], left, turned, right, size, before))

    for h in range(lane_rows):
        gathered[place, pl.ds(h, 1), :] = row_of(totals, *tables[h])

    def give(at, row=place):
        pltpu.make_async_remote_copy(
            src_ref=gathered.at[row], dst_ref=gathered.at[row], send_sem=s_send.at[0],
            recv_sem=a_recv.at[0], device_id=at, device_id_type=MESH).start()

    for root in range(nroots):
        @pl.when((place != root * ngy) & jnp.logical_not(is_served & helped))
        def _():
            give((0, root, 0))
    pl.when(jnp.logical_not(early))(meet_depth)
    pl.when(inner)(meet_across)

    pl.semaphore_wait(plane_sem.at[0], nta - 1)
    each(ranks, place, nroots, give)
    if helped:
        @pl.when(is_helper)
        def _():
            def sides(slot):
                own = pl.ds(slot * 6 * size, 6 * size)
                return heap_left.at[own], heap_turned.at[own]

            first = []
            for z in served:
                slot = z // 2
                bytes_of = heap_left.at[pl.ds(0, (3 if slot == 0 else 6) * size + 9)]
                pltpu.make_async_copy(bytes_of, bytes_of, heap_recv.at[slot]).wait()
                first.append(self_sums(heap.at[z], *sides(slot), size))
                carry_link(heap.at[z], link_at(heap_links.at[slot]), *sides(slot), size)
            for z in reversed(served):
                slot, other = z // 2, (z + 1) % ngz

                def before(c):
                    for i, piece in enumerate(PIECES):
                        if c == piece[0] and slot == 0:
                            part = heap.at[other, :, pl.ds(*piece)]
                            pltpu.make_async_copy(part, part, heap_recv.at[len(served) + i]).wait()

                pair = pair_sums(heap.at[other], *sides(slot), right, size, before)
                for h in range(lane_rows):
                    gathered[place_of(z), pl.ds(h, 1), :] = row_of(
                        [first[slot], pair], heap_tables[slot, h], tables[h][1])
                for root in range(nroots - 1):
                    give((0, root, 0), place_of(z))

    def rows_done(semaphore, rows):
        if rows > 0:
            pltpu.make_async_copy(gathered.at[pl.ds(0, rows)], gathered.at[pl.ds(0, rows)], semaphore).wait()

    mine = len(served)
    for copy in link_sends:
        copy.wait_send()
    pltpu.make_async_copy(far, far, s_send.at[0]).wait()
    if helped:
        @pl.when(is_distant)
        def _():
            pltpu.make_async_copy(near, near, s_send.at[0]).wait()

        @pl.when(is_served)
        def _():
            pltpu.make_async_copy(near_links, near_links, s_send.at[0]).wait()

        pl.when(is_helper)(lambda: rows_done(s_send.at[0], mine * (nroots - 1)))
        pl.when(jnp.logical_not(is_served))(lambda: rows_done(s_send.at[0], nroots))
        rows_done(s_send.at[0], count - 1 - nroots)
    else:
        rows_done(s_send.at[0], count - 1)
    if helped:
        pl.when(is_helper)(lambda: rows_done(a_recv.at[0], count - 1 - mine))
        pl.when(jnp.logical_not(is_helper))(lambda: rows_done(a_recv.at[0], count - 1))
    else:
        rows_done(a_recv.at[0], count - 1)
    for t in range(nta):
        for h in range(lane_rows):
            total = row_sum(gathered, t * ngz * ngy, ngz * ngy, h)
            low = h * (LANES // np_)
            for row in range(low, min(low + LANES // np_, out.shape[1]), 8):
                shift = (1 + row - low) * np_
                out[t, pl.ds(row, 8), :] = pltpu.roll(total, shift, 1, stride=np_, stride_axis=0)[:, :np_]


def row_sum(ref, start, size, h):
    if size > 32:
        total = jnp.sum(ref[pl.ds(start, size), pl.ds(h, 1), :], axis=0)
        return jnp.broadcast_to(total, (8, LANES))
    terms = [jnp.broadcast_to(ref[start + i, pl.ds(h, 1), :], (8, LANES)) for i in range(size)]
    while len(terms) > 1:
        terms = [sum(terms[i:i + 2]) for i in range(0, len(terms), 2)]
    return terms[0]


def each(ranks, place, start, act):
    nta, ngz, ngy = ranks
    count = nta * ngz * ngy

    def one(step, along):
        beside = step // (nta * ngz)
        across = step // ngz % nta

        @pl.when(place != (across * ngz + along) * ngy + beside)
        def _():
            act((across, along, beside))

    if count > 64:
        lax.fori_loop(start, count, lambda step, carry: (one(step, step % ngz), carry)[1], 0)
        return
    for step in range(start, count):
        one(step, step % ngz)


def body(ranks, propagator, links, source_z, displacements, momenta, gamma_perm, gamma_phase):
    nta, ngz, ngy = ranks
    sites = propagator.shape[6]
    ndisp, np_, ng = displacements.shape[0], momenta.shape[0], gamma_perm.shape[0]
    nsteps = (ndisp - 1) // 2
    sizes = (ndisp, ng, np_, ngz)
    scaling = 1.0 / (24.0 * math.sqrt(sites * ngy * ngz))
    field = jnp.transpose(propagator, (0, 2, 3, 4, 5, 1, 6)).reshape(2, 3, -1, sites)
    link = jnp.transpose(links, (1, 2, 3, 4, 0, 5)).reshape(9, 2, sites)
    size = field.shape[2]
    regular = pltpu.SemaphoreType.REGULAR
    lane_rows = -(-ndisp * ng * np_ * 2 // LANES)
    more = max(nsteps - 1, 1)
    dma = pltpu.SemaphoreType.DMA
    helped = nsteps == 1 and ngz == 4 and nta * ngy > 1
    pairs = ngz // 2
    heaps = [
        pltpu.VMEM((ngz, 2, 3, size, sites), jnp.bfloat16),
        pltpu.VMEM((pairs, 9, 2, sites), jnp.bfloat16),
        pltpu.VMEM((pairs * 6 * size, sites), jnp.float32),
        pltpu.VMEM((pairs * 6 * size, sites), jnp.float32),
        pltpu.VMEM((pairs, lane_rows, 32, LANES), jnp.float32),
    ] if helped else []
    heap_sems = [dma((pairs + len(PIECES),))] if helped else []
    reduced = pl.pallas_call(
        functools.partial(kernel, sizes, scaling, ranks, helped),
        out_shape=pltpu.VMEM((nta, ndisp * ng * 2, np_), jnp.float32),
        in_specs=[pl.BlockSpec(memory_space=pltpu.HBM)] * 7,
        out_specs=pl.BlockSpec(memory_space=pltpu.VMEM),
        scratch_shapes=[
            pltpu.VMEM((2, 3, size, sites), jnp.bfloat16),
            pltpu.VMEM((9, 2, sites), jnp.bfloat16),
            pltpu.VMEM((nsteps, 2, 3, size, sites), jnp.bfloat16),
            pltpu.VMEM((more, 9, 2, sites), jnp.bfloat16),
            pltpu.VMEM((6 * size, sites), jnp.float32),
            pltpu.VMEM((6 * size, sites), jnp.float32),
            pltpu.VMEM((6 * size, sites), jnp.float32),
            *heaps,
            pltpu.SMEM(source_z.shape, jnp.int32),
            pltpu.SMEM(displacements.shape, jnp.int32),
            pltpu.SMEM(momenta.shape, jnp.int32),
            pltpu.SMEM(gamma_perm.shape, jnp.int32),
            pltpu.SMEM(gamma_phase.shape, jnp.int32),
            pltpu.VMEM((nta * ngz * ngy, lane_rows, LANES), jnp.float32),
            dma((3,)), dma((1,)), dma((nsteps, len(PIECES))),
            dma((1,)), regular((1,)), regular((1,)), regular((1,)),
            *heap_sems,
        ] + [dma((nsteps - 1,))] * (2 if nsteps > 1 else 0),
        compiler_params=pltpu.CompilerParams(collective_id=0, has_side_effects=True),
    )(field, link, source_z, displacements, momenta, gamma_perm, gamma_phase)
    return jnp.swapaxes(reduced.reshape(nta, ndisp, ng, 2, np_), 3, 4)


def solution(mesh):
    placed = (
        P(None, None, None, None, "ta", "gz", "gy"),
        P(None, None, None, "ta", "gz", "gy"),
        P(),
        P(),
        P(),
        P(),
        P(),
    )
    ranks = tuple(mesh.shape[axis] for axis in ("ta", "gz", "gy"))
    return jax.shard_map(
        functools.partial(body, ranks), mesh=mesh, in_specs=placed, out_specs=P(), check_vma=False
    )
```

```python
import functools
import math

import jax
import jax.numpy as jnp
from jax import lax
from jax.experimental import pallas as pl
from jax.experimental.pallas import tpu as pltpu
from jax.sharding import PartitionSpec as P

MESH = pl.DeviceIdType.MESH
PIECES = ((0, 2), (2, 1))
LANES = 128


def weights(lane_row, sizes, smem, place, scaling):
    ndisp, ng, np_, nz = sizes
    src, disp, mom, perm, phase = smem
    slice_at, depth_at = place
    nsteps = (ndisp - 1) // 2
    shape = (32, LANES)
    lane = lax.broadcasted_iota(jnp.int32, shape, 1)
    momentum = lane & (np_ - 1)
    lane = lane_row * LANES + LANES - np_ - (lane - momentum)
    row = lax.broadcasted_iota(jnp.int32, shape, 0)
    out_part = (lane // np_) & 1
    gamma = (lane // (2 * np_)) & (ng - 1)
    entry = lane // (2 * np_ * ng)
    in_part = row // 16
    second = row & 3
    first = (second - row // 4) & 3
    reach = jnp.full(shape, 2 * nsteps + 1, jnp.int32)
    for j in range(ndisp):
        reach = jnp.where(entry == j, disp[j] - nsteps, reach)
    backward = reach < 0
    momenta = jnp.zeros(shape, jnp.int32)
    source = jnp.zeros(shape, jnp.int32)
    for p in range(np_):
        momenta = jnp.where(momentum == p, mom[p], momenta)
        source = jnp.where(momentum == p, src[slice_at, p], source)
    depth = depth_at - jnp.where(backward, reach, 0)
    turns = (momenta * (depth - source)).astype(jnp.float32) * (1.0 / nz)
    angle = (turns - jnp.floor(turns)) * (2.0 * math.pi)
    cosine = jnp.cos(angle)
    sine = jnp.sin(angle)
    sink = jnp.where(backward, second, first)
    other = jnp.where(backward, first, second)
    column = jnp.zeros(shape, jnp.int32)
    power = jnp.zeros(shape, jnp.int32)
    for g in range(ng):
        for s in range(4):
            here = (gamma == g) & (sink == s)
            column = jnp.where(here, perm[g, s], column)
            power = jnp.where(here, phase[g, s], power)
    quarter = power - out_part + jnp.where(backward, -in_part, in_part)
    quarter = quarter & 3
    value = jnp.where((quarter & 1) == 0, cosine, sine)
    value = jnp.where(quarter >= 2, -value, value)
    value = jnp.where((column == other) & (entry < ndisp), value * scaling, 0.0)
    return value, jnp.abs(reach)


def add_pairs(sums, left, turned, right, start, size):
    def rows(ref, s):
        return ref[pl.ds(start + s, size // 4, stride=4), :].reshape(-1, 8, LANES)

    rights = [rows(right, u) for u in range(4)]
    out = []
    for side in (left, turned):
        for s in range(4):
            own = rows(side, s)
            out += [jnp.sum(own * other, axis=0) for other in rights]
    return out if sums is None else [x + y for x, y in zip(sums, out)]


def site_sums(sums):
    row = lax.broadcasted_iota(jnp.int32, (8, LANES), 0)
    for step in (1, 2, 4):
        first = (row & step) == 0
        pairs = zip(sums[::2], sums[1::2])
        sums = [
            jnp.where(first, x, y) + pltpu.roll(jnp.where(first, y, x), step, 0)
            for x, y in pairs
        ]
    return jnp.sum(jnp.concatenate(sums, axis=0), axis=1, keepdims=True)


def lane_sums(halves):
    row = lax.broadcasted_iota(jnp.int32, (8, LANES), 0)
    folded = [
        jnp.where(row < 4, x, y) + pltpu.roll(jnp.where(row < 4, y, x), 4, 0)
        for x, y in zip(halves[::2], halves[1::2])
    ]
    return jnp.sum(jnp.concatenate(folded, axis=0), axis=1, keepdims=True)


def spins_turned(x, steps):
    if steps == 0:
        return x
    spin = lax.broadcasted_iota(jnp.int32, x.shape, 1) & 3
    return jnp.where(spin >= steps, pltpu.roll(x, steps, 1), pltpu.roll(x, steps + 4, 1))


def keep(left, turned, at, size, real, imag):
    real, imag = real.reshape(-1, LANES), imag.reshape(-1, LANES)
    left[pl.ds(at, size), :] = real
    left[pl.ds(at + size, size), :] = imag
    turned[pl.ds(at, size), :] = -imag
    turned[pl.ds(at + size, size), :] = real


def self_sums(field, left, turned, size):
    sums = None
    for c in range(3):
        keep(left, turned, 2 * size * c, size, field[0, c].astype(jnp.float32), field[1, c].astype(jnp.float32))
        sums = add_pairs(sums, left, turned, left, 2 * size * c, 2 * size)
    return site_sums([
        sums[16 * side + 4 * ((u - d) % 4) + u] for side in range(2) for d in range(4) for u in range(4)
    ])


def link_at(ref):
    return [
        [
            [jnp.broadcast_to(ref[3 * a + b, pl.ds(part, 1), :].astype(jnp.float32), (8, LANES))
             for part in range(2)]
            for b in range(3)
        ]
        for a in range(3)
    ]


def carry_link(near, wilson, sides, size):
    for chunk in range(size // 16):
        field = [
            [
                near[part, a, pl.ds(chunk * 16, 16), :].astype(jnp.float32).reshape(2, 8, LANES)
                for a in range(3)
            ]
            for part in range(2)
        ]
        for b in range(3):
            real = sum(field[0][a] * wilson[a][b][0] + field[1][a] * wilson[a][b][1] for a in range(3))
            imag = sum(field[1][a] * wilson[a][b][0] - field[0][a] * wilson[a][b][1] for a in range(3))
            for d in range(4):
                re = spins_turned(real, d).reshape(16, LANES)
                im = spins_turned(imag, d).reshape(16, LANES)
                at = 6 * size * d + 2 * size * b + chunk * 16
                sides[pl.ds(at, 16), :] = re
                sides[pl.ds(at + size, 16), :] = im
                sides[pl.ds(24 * size + at, 16), :] = -im
                sides[pl.ds(24 * size + at + size, 16), :] = re


def pair_sums(far, sides, size, before):
    sums = None
    for c in range(3):
        before(c)
        right = jnp.concatenate([far[part, c].astype(jnp.float32) for part in range(2)], axis=0)
        right = right.reshape(-1, 8, LANES)
        more = [
            jnp.sum(sides[pl.ds(6 * size * v + 2 * size * c, 2 * size), :].reshape(-1, 8, LANES) * right, axis=0)
            for v in range(8)
        ]
        sums = more if sums is None else [x + y for x, y in zip(sums, more)]
    return lane_sums(sums)


def row_of(totals, table, reach):
    chosen = jnp.zeros(table.shape, jnp.float32)
    for k, total in enumerate(totals):
        chosen = jnp.where(reach == k, total, chosen)
    return jnp.sum(chosen * table, axis=0, keepdims=True)


def kernel(sizes, scaling, ranks, helped, *refs):
    refs = list(refs)
    prop, links, src_h, disp_h, mom_h, perm_h, phase_h, out = refs[:8]
    near, near_links, far, far_links, left, turned, sides = refs[8:15]
    rest = refs[15:]
    heap = heap_links = heap_sides = heap_tables = None
    if helped:
        heap, heap_links, heap_sides, heap_tables = rest[:4]
        rest = rest[4:]
    src, disp, mom, perm, phase, gathered = rest[:6]
    local_sem, s_send, s_recv, a_recv, low_sem, line_sem, plane_sem = rest[6:13]
    rest = rest[13:]
    heap_recv = None
    if helped:
        heap_recv, rest = rest[0], rest[1:]
    link_sems = rest
    ndisp, ng, np_, nz = sizes
    nta, ngz, ngy = ranks
    nsteps = (ndisp - 1) // 2
    size = near.shape[2]
    lane_rows = gathered.shape[1]
    ta, gz, gy = lax.axis_index("ta"), lax.axis_index("gz"), lax.axis_index("gy")
    place = (ta * ngz + gz) * ngy + gy

    loads = [
        pltpu.make_async_copy(a, b, local_sem.at[min(i, 2)])
        for i, (a, b) in enumerate(
            [(prop.at[:, c], near.at[:, c]) for c in range(3)] + [(links, near_links)]
        )
    ]
    smalls = [
        pltpu.make_async_copy(a, b, local_sem.at[0])
        for a, b in [(src_h, src), (disp_h, disp), (mom_h, mom), (perm_h, perm), (phase_h, phase)]
    ]

    lines = [
        (gz, ngz, lambda i: (ta, i, gy)),
        (gy, ngy, lambda i: (ta, gz, i)),
        (ta, nta, lambda i: (i, gz, gy)),
    ]

    def greet(semaphore, at):
        pl.semaphore_signal(semaphore, inc=1, device_id=at, device_id_type=MESH)

    def greet_span(semaphore, line, low, high):
        lax.fori_loop(low, high, lambda i, carry: (greet(semaphore, line[2](i)), carry)[1], 0)

    def greet_line(semaphore, line):
        greet_span(semaphore, line, 0, line[0])
        greet_span(semaphore, line, line[0] + 1, line[1])

    count = nta * ngz * ngy
    barrier = pltpu.get_barrier_semaphore()
    for k in range(1, nsteps + 1):
        @pl.when(gz + k >= ngz)
        def _():
            greet(barrier, (ta, gz + k - ngz, gy))
    for load in loads:
        load.start()
    for line in lines:
        greet_span(barrier, line, line[0] + 1, line[1])
    nroots = min(2, ngz)
    is_root = (ta + gy == 0) & (gz < nroots)
    helper_at = (0, nroots - 1, 0)
    is_helper = (ta + gy == 0) & (gz == nroots - 1)
    is_distant = (ta == nta - 1) & (gy == ngy - 1)
    inner = lax.rem(gz, 2) == 0
    is_served = is_distant & jnp.logical_not(inner)
    served = list(range(1, ngz, 2)) if helped else []

    def place_of(z):
        return ((nta - 1) * ngz + z) * ngy + ngy - 1

    @pl.when(is_root)
    def _():
        def one(step, carry):
            at = (step // (ngz * ngy), step // ngy % ngz, step % ngy)

            @pl.when(step != place)
            def _():
                greet(barrier, at)

            return carry

        lax.fori_loop(0, count, one, 0)

    pl.semaphore_wait(
        barrier,
        jnp.maximum(gz, nsteps) + gy + ta + nroots - jnp.where(is_root, 1, 0),
    )

    def target(k):
        return (ta, lax.rem(gz + ngz - k, ngz), gy)

    sends = [
        [
            pltpu.make_async_remote_copy(
                src_ref=near.at[:, c], dst_ref=far.at[k - 1, :, c], send_sem=s_send.at[0],
                recv_sem=s_recv.at[k - 1, c // 2], device_id=target(k), device_id_type=MESH)
            for c in range(3)
        ]
        for k in range(1, nsteps + 1)
    ]
    u_send, u_recv = link_sems if link_sems else (None, None)
    link_sends = [
        pltpu.make_async_remote_copy(
            src_ref=near_links, dst_ref=far_links.at[k - 1], send_sem=u_send.at[k - 1],
            recv_sem=u_recv.at[k - 1], device_id=target(k), device_id_type=MESH)
        for k in range(1, nsteps)
    ]

    def to_helper(source, slot, semaphore):
        pltpu.make_async_remote_copy(
            src_ref=source, dst_ref=slot, send_sem=s_send.at[0], recv_sem=heap_recv.at[semaphore],
            device_id=helper_at, device_id_type=MESH).start()

    def field_semaphore(c):
        slot = jnp.where(inner, lax.rem(gz + ngz - 1, ngz), gz) // 2
        return jnp.where(inner & (slot == 0), len(served) + c // 2, slot)

    for c in range(3):
        loads[c].wait()
        if c == 2:
            loads[3].wait()
        for copies in sends:
            copies[c].start()
        if helped:
            pl.when(is_distant)(
                lambda: to_helper(near.at[:, c], heap.at[gz, :, c], field_semaphore(c)))
    for line in lines:
        greet_span(low_sem.at[0], line, 0, line[0])
    if helped:
        @pl.when(is_served)
        def _():
            to_helper(near_links, heap_links.at[gz // 2], gz // 2)
    for small in smalls:
        small.start()
    for copy in link_sends:
        copy.start()
    totals = [self_sums(near, left, turned, size)]
    for small in smalls:
        small.wait()
    later = (ngz - 1 - gz) + (ngy - 1 - gy) + (nta - 1 - ta)
    outer = jnp.logical_not(inner)
    early = outer | (gy == ngy - 1)

    def meet_depth():
        @pl.when(later > 0)
        def _():
            pl.semaphore_wait(low_sem.at[0], later)

        greet_line(line_sem.at[0], lines[0])

    def meet_across():
        pl.semaphore_wait(line_sem.at[0], ngz - 1)
        greet_line(plane_sem.at[0], lines[2])

    pl.when(early)(meet_depth)
    tables = [
        weights(h, sizes, (src, disp, mom, perm, phase), (ta, gz), scaling)
        for h in range(lane_rows)
    ]

    if helped:
        @pl.when(is_helper)
        def _():
            for z in served:
                for h in range(lane_rows):
                    heap_tables[z // 2, h] = weights(
                        h, sizes, (src, disp, mom, perm, phase), (nta - 1, z), scaling)[0]

    wilson = None
    for k in range(1, nsteps + 1):
        if k == 1:
            wilson = link_at(near_links)
        else:
            link_sends[k - 2].wait_recv()
            step = link_at(far_links.at[k - 2])
            wilson = [
                [
                    [
                        sum(wilson[a][c][0] * step[c][b][0] - wilson[a][c][1] * step[c][b][1] for c in range(3)),
                        sum(wilson[a][c][0] * step[c][b][1] + wilson[a][c][1] * step[c][b][0] for c in range(3)),
                    ]
                    for b in range(3)
                ]
                for a in range(3)
            ]
        carry_link(near, wilson, sides, size)

        def before(c):
            for i, piece in enumerate(PIECES):
                if c == piece[0]:
                    if k == nsteps and i == len(PIECES) - 1:
                        pl.when(outer)(meet_across)
                    part = far.at[k - 1, :, pl.ds(*piece)]
                    pltpu.make_async_copy(part, part, s_recv.at[k - 1, i]).wait()

        totals.append(pair_sums(far.at[k - 1], sides, size, before))

    for h in range(lane_rows):
        gathered[place, pl.ds(h, 1), :] = row_of(totals, *tables[h])

    def give(at, row=place):
        pltpu.make_async_remote_copy(
            src_ref=gathered.at[row], dst_ref=gathered.at[row], send_sem=s_send.at[0],
            recv_sem=a_recv.at[0], device_id=at, device_id_type=MESH).start()

    for root in range(nroots):
        @pl.when((place != root * ngy) & jnp.logical_not(is_served & helped))
        def _():
            give((0, root, 0))
    pl.when(jnp.logical_not(early))(meet_depth)
    pl.when(inner)(meet_across)

    pl.semaphore_wait(plane_sem.at[0], nta - 1)
    each(ranks, place, nroots, give)
    if helped:
        @pl.when(is_helper)
        def _():
            def own(slot):
                return heap_sides.at[pl.ds(slot * 48 * size, 48 * size)]

            first = []
            for z in served:
                slot = z // 2
                bytes_of = heap_sides.at[pl.ds(0, (3 if slot == 0 else 6) * size + 9)]
                pltpu.make_async_copy(bytes_of, bytes_of, heap_recv.at[slot]).wait()
                first.append(self_sums(heap.at[z], left, turned, size))
                carry_link(heap.at[z], link_at(heap_links.at[slot]), own(slot), size)
            for z in reversed(served):
                slot, other = z // 2, (z + 1) % ngz

                def before(c):
                    for i, piece in enumerate(PIECES):
                        if c == piece[0] and slot == 0:
                            part = heap.at[other, :, pl.ds(*piece)]
                            pltpu.make_async_copy(part, part, heap_recv.at[len(served) + i]).wait()

                pair = pair_sums(heap.at[other], own(slot), size, before)
                for h in range(lane_rows):
                    gathered[place_of(z), pl.ds(h, 1), :] = row_of(
                        [first[slot], pair], heap_tables[slot, h], tables[h][1])
                for root in range(nroots - 1):
                    give((0, root, 0), place_of(z))

    def rows_done(semaphore, rows):
        if rows > 0:
            pltpu.make_async_copy(gathered.at[pl.ds(0, rows)], gathered.at[pl.ds(0, rows)], semaphore).wait()

    mine = len(served)
    for copy in link_sends:
        copy.wait_send()
    pltpu.make_async_copy(far, far, s_send.at[0]).wait()
    if helped:
        @pl.when(is_distant)
        def _():
            pltpu.make_async_copy(near, near, s_send.at[0]).wait()

        @pl.when(is_served)
        def _():
            pltpu.make_async_copy(near_links, near_links, s_send.at[0]).wait()

        pl.when(is_helper)(lambda: rows_done(s_send.at[0], mine * (nroots - 1)))
        pl.when(jnp.logical_not(is_served))(lambda: rows_done(s_send.at[0], nroots))
        rows_done(s_send.at[0], count - 1 - nroots)
    else:
        rows_done(s_send.at[0], count - 1)
    if helped:
        pl.when(is_helper)(lambda: rows_done(a_recv.at[0], count - 1 - mine))
        pl.when(jnp.logical_not(is_helper))(lambda: rows_done(a_recv.at[0], count - 1))
    else:
        rows_done(a_recv.at[0], count - 1)
    for t in range(nta):
        for h in range(lane_rows):
            total = row_sum(gathered, t * ngz * ngy, ngz * ngy, h)
            low = h * (LANES // np_)
            for row in range(low, min(low + LANES // np_, out.shape[1]), 8):
                shift = (1 + row - low) * np_
                out[t, pl.ds(row, 8), :] = pltpu.roll(total, shift, 1, stride=np_, stride_axis=0)[:, :np_]


def row_sum(ref, start, size, h):
    if size > 32:
        total = jnp.sum(ref[pl.ds(start, size), pl.ds(h, 1), :], axis=0)
        return jnp.broadcast_to(total, (8, LANES))
    terms = [jnp.broadcast_to(ref[start + i, pl.ds(h, 1), :], (8, LANES)) for i in range(size)]
    while len(terms) > 1:
        terms = [sum(terms[i:i + 2]) for i in range(0, len(terms), 2)]
    return terms[0]


def each(ranks, place, start, act):
    nta, ngz, ngy = ranks
    count = nta * ngz * ngy

    def one(step, along):
        beside = step // (nta * ngz)
        across = step // ngz % nta

        @pl.when(place != (across * ngz + along) * ngy + beside)
        def _():
            act((across, along, beside))

    if count > 64:
        lax.fori_loop(start, count, lambda step, carry: (one(step, step % ngz), carry)[1], 0)
        return
    for step in range(start, count):
        one(step, step % ngz)


def body(ranks, propagator, links, source_z, displacements, momenta, gamma_perm, gamma_phase):
    nta, ngz, ngy = ranks
    sites = propagator.shape[6]
    ndisp, np_, ng = displacements.shape[0], momenta.shape[0], gamma_perm.shape[0]
    nsteps = (ndisp - 1) // 2
    sizes = (ndisp, ng, np_, ngz)
    scaling = 1.0 / (24.0 * math.sqrt(sites * ngy * ngz))
    field = jnp.transpose(propagator, (0, 2, 3, 4, 5, 1, 6)).reshape(2, 3, -1, sites)
    link = jnp.transpose(links, (1, 2, 3, 4, 0, 5)).reshape(9, 2, sites)
    size = field.shape[2]
    regular = pltpu.SemaphoreType.REGULAR
    lane_rows = -(-ndisp * ng * np_ * 2 // LANES)
    more = max(nsteps - 1, 1)
    dma = pltpu.SemaphoreType.DMA
    helped = nsteps == 1 and ngz == 4 and nta * ngy > 1
    pairs = ngz // 2
    heaps = [
        pltpu.VMEM((ngz, 2, 3, size, sites), jnp.bfloat16),
        pltpu.VMEM((pairs, 9, 2, sites), jnp.bfloat16),
        pltpu.VMEM((pairs * 48 * size, sites), jnp.float32),
        pltpu.VMEM((pairs, lane_rows, 32, LANES), jnp.float32),
    ] if helped else []
    heap_sems = [dma((pairs + len(PIECES),))] if helped else []
    reduced = pl.pallas_call(
        functools.partial(kernel, sizes, scaling, ranks, helped),
        out_shape=pltpu.VMEM((nta, ndisp * ng * 2, np_), jnp.float32),
        in_specs=[pl.BlockSpec(memory_space=pltpu.HBM)] * 7,
        out_specs=pl.BlockSpec(memory_space=pltpu.VMEM),
        scratch_shapes=[
            pltpu.VMEM((2, 3, size, sites), jnp.bfloat16),
            pltpu.VMEM((9, 2, sites), jnp.bfloat16),
            pltpu.VMEM((nsteps, 2, 3, size, sites), jnp.bfloat16),
            pltpu.VMEM((more, 9, 2, sites), jnp.bfloat16),
            pltpu.VMEM((6 * size, sites), jnp.float32),
            pltpu.VMEM((6 * size, sites), jnp.float32),
            pltpu.VMEM((48 * size, sites), jnp.float32),
            *heaps,
            pltpu.SMEM(source_z.shape, jnp.int32),
            pltpu.SMEM(displacements.shape, jnp.int32),
            pltpu.SMEM(momenta.shape, jnp.int32),
            pltpu.SMEM(gamma_perm.shape, jnp.int32),
            pltpu.SMEM(gamma_phase.shape, jnp.int32),
            pltpu.VMEM((nta * ngz * ngy, lane_rows, LANES), jnp.float32),
            dma((3,)), dma((1,)), dma((nsteps, len(PIECES))),
            dma((1,)), regular((1,)), regular((1,)), regular((1,)),
            *heap_sems,
        ] + [dma((nsteps - 1,))] * (2 if nsteps > 1 else 0),
        compiler_params=pltpu.CompilerParams(collective_id=0, has_side_effects=True),
    )(field, link, source_z, displacements, momenta, gamma_perm, gamma_phase)
    return jnp.swapaxes(reduced.reshape(nta, ndisp, ng, 2, np_), 3, 4)


def solution(mesh):
    placed = (
        P(None, None, None, None, "ta", "gz", "gy"),
        P(None, None, None, "ta", "gz", "gy"),
        P(),
        P(),
        P(),
        P(),
        P(),
    )
    ranks = tuple(mesh.shape[axis] for axis in ("ta", "gz", "gy"))
    return jax.shard_map(
        functools.partial(body, ranks), mesh=mesh, in_specs=placed, out_specs=P(), check_vma=False
    )
```
